1024 devices in a mesh: section: 8 (over x, core), row: 8 (over y), col: 16 (over z).
Axes of the slice: x: 4, y: 8, z: 16, core: 2. Of those that a mesh axis runs over, the one named last changes fastest.
Arguments:
- hidden: bfloat16 [4, 32, 4096], P(None, None, 'col'), may hold values from -6 to 6
- norm_gain: bfloat16 [8, 4096], P('section', 'col'), may hold values from 0.25 to 1.75
- w_qkv: bfloat16 [8, 4096, 6144], P('section', 'col', 'row'), may hold values from -0.09375 to 0.09375
- w_out: bfloat16 [8, 4096, 4096], P('section', 'row', 'col'), may hold values from -0.09375 to 0.09375
- cache_keys: bfloat16 [8, 4, 32, 128, 8, 128], P('section', None, 'col', None, 'row'), may hold values from -240 to 240, as said below
- cache_values: bfloat16 [8, 4, 32, 128, 8, 128], P('section', None, 'col', None, 'row'), may hold values from -6 to 6
- cache_lengths: int32 [4, 32], P(None, 'col'), may hold values from 1 to 127
Outputs:
- layer_outputs: bfloat16 [8, 4, 32, 4096], P('section', None, None, 'col')
The draws below stay inside these ranges and needn't reach their ends.
Inputs may be any that keep to these rules, and one draw needn't show every extreme that they name: `cache_keys`: cached keys are of order one except that some sequences may carry much larger keys at a few positions.
All inputs are finite; a program needn't handle non-finite values.
Results may differ from the reference program's by a relative error of at most 0.04.
Values may be sent and summed in bfloat16 or wider, within the bound.
A program may use at most 32 MiB of HBM per device.

```python
import jax
import jax.numpy as jnp
from jax import lax

D = 4096
HEADS = 32
KVH = 8
HD = 128
MICRO = 4
LEN = 128
LAYERS = 8
BATCH = 32


def draw_cache_keys(key, part):
    normal_draw = jnp.clip(jax.random.normal(key, (LAYERS, MICRO, BATCH, LEN, KVH, HD), jnp.float32), -6.0, 6.0)
    return normal_draw.astype(jnp.bfloat16)


def touch_ends(drawn, rng, low, top_value):
    extent = drawn.shape
    spot = [jax.random.randint(jax.random.fold_in(rng, axis), (), 0, extent[axis]) for axis in range(len(extent))]
    drawn = drawn.at[tuple(spot)].set(low)
    longest = extent.index(max(extent))
    spot[longest] = (spot[longest] + 1) % extent[longest]
    return drawn.at[tuple(spot)].set(top_value)


def steps_of(rng, extent, pieces, smallest, top_value):
    loudness, own = 1.0, jax.random.fold_in(rng, 6)
    for position, blocks in pieces:
        draws = jnp.exp(jax.random.uniform(jax.random.fold_in(own, position), (blocks,), jnp.float32, smallest / len(pieces), top_value / len(pieces)))
        loudness = loudness * jnp.repeat(draws, extent[position] // blocks).reshape([-1 if axis == position else 1 for axis in range(len(extent))])
    return loudness


def noise(stream_key, extent, width, limit, cuts=(), kind=jnp.bfloat16):
    array = jax.random.normal(stream_key, extent, jnp.float32) * width
    if len(cuts) > 0:
        array = steps_of(stream_key, extent, cuts, -0.22, 0.18) * array
    return jnp.clip(array, min=-limit, max=limit).astype(kind)


def setup_inputs(seed: int = 0) -> dict:
    seeds = jax.random.split(jax.random.key(seed), 8)
    hidden = noise(seeds[0], (MICRO, BATCH, D), 1.0, 6.0, ((2, 16),))
    norm_gain = jnp.clip(1.0 + 0.15 * jax.random.normal(seeds[1], (LAYERS, D), jnp.float32), 0.25, 1.75).astype(jnp.bfloat16)
    w_qkv = noise(seeds[2], (LAYERS, D, (HEADS + 2 * KVH) * HD), D ** -0.5, 0.09375, ((0, 8), (1, 16), (2, 8)))
    w_out = noise(seeds[3], (LAYERS, HEADS * HD, D), (HEADS * HD) ** -0.5, 0.09375, ((0, 8), (1, 8), (2, 16)))
    cache_keys = draw_cache_keys(jax.random.fold_in(seeds[7], 71), 0)
    cache_values = noise(seeds[5], (LAYERS, MICRO, BATCH, LEN, KVH, HD), 1.0, 6.0, ((0, 8), (2, 16), (4, 8)))
    cache_lengths = touch_ends(jax.random.randint(seeds[6], (MICRO, BATCH), 1, LEN), jax.random.fold_in(seeds[6], 1), 1, LEN - 1).astype(jnp.int32)
    return {"hidden": hidden, "norm_gain": norm_gain, "w_qkv": w_qkv, "w_out": w_out, "cache_keys": cache_keys, "cache_values": cache_values, "cache_lengths": cache_lengths}


def rotate(vectors, positions):
    half_dim = vectors.shape[-1] // 2
    inverse_freq = 500000.0 ** (-jnp.arange(half_dim, dtype=jnp.float32) * 2.0 / vectors.shape[-1])
    angles = positions * inverse_freq
    angles = jnp.concatenate([angles, angles], axis=-1)
    swapped = jnp.concatenate([-vectors[..., half_dim:], vectors[..., :half_dim]], axis=-1)
    return vectors * jnp.cos(angles) + swapped * jnp.sin(angles)

def attend(queries, new_key, new_value, key_block, value_block, length):
    score_scale = 1.0 / jnp.sqrt(jnp.float32(queries.shape[-1]))
    scores = jnp.einsum('bgrd,bjgd->bgrj', queries.astype(jnp.float32), key_block.astype(jnp.float32)) * score_scale
    own_score = jnp.einsum('bgrd,bgd->bgr', queries.astype(jnp.float32), new_key.astype(jnp.float32)) * score_scale
    visible = jnp.arange(key_block.shape[1])[None, :] < length[:, None]
    scores = jnp.where(visible[:, None, None, :], scores, -jnp.inf)
    row_max = jnp.maximum(lax.optimization_barrier(jnp.max(scores, axis=-1)), own_score)
    cache_exp = jnp.exp(scores - row_max[..., None])
    own_exp = jnp.exp(own_score - row_max)
    total = lax.optimization_barrier(jnp.sum(cache_exp, axis=-1)) + own_exp
    cache_weight = (cache_exp / total[..., None]).astype(jnp.bfloat16)
    own_weight = (own_exp / total).astype(jnp.bfloat16)
    result = jnp.einsum('bgrj,bjgd->bgrd', cache_weight.astype(jnp.float32), value_block.astype(jnp.float32))
    result = result + own_weight.astype(jnp.float32)[..., None] * new_value.astype(jnp.float32)[:, :, None, :]
    return result.astype(jnp.bfloat16)

def heads_part(projected, key_block, value_block, length):
    per_group = projected.shape[2] - 2
    positions = length.astype(jnp.float32)
    queries = rotate(projected[:, :, :per_group], positions[:, None, None, None]).astype(jnp.bfloat16)
    new_key = rotate(projected[:, :, per_group], positions[:, None, None]).astype(jnp.bfloat16)
    new_value = projected[:, :, per_group + 1].astype(jnp.bfloat16)
    attended = attend(queries, new_key, new_value, key_block, value_block, length)
    return attended.reshape(attended.shape[0], -1)

def decoder_layer(current, gain_row, proj_weight, out_weight, key_block, value_block, length):
    h_float = current.astype(jnp.float32)
    scaled = (h_float * gain_row.astype(jnp.float32)).astype(jnp.bfloat16)
    squares = lax.optimization_barrier(jnp.sum(h_float * h_float, axis=1))
    factor = lax.rsqrt(squares / D + 1e-05)
    projected = jnp.dot(scaled, proj_weight, preferred_element_type=jnp.float32) * factor[:, None]
    projected = projected.reshape(current.shape[0], KVH, HEADS // KVH + 2, HD)
    attended = heads_part(projected, key_block, value_block, length)
    mixed_rows = jnp.dot(attended, out_weight, preferred_element_type=jnp.float32)
    return (h_float + mixed_rows).astype(jnp.bfloat16)

def reference(hidden, norm_gain, w_qkv, w_out, cache_keys, cache_values, cache_lengths):
    current = hidden
    collected = []
    for layer_at in range(LAYERS):
        produced = []
        for micro_at in range(MICRO):
            produced.append(decoder_layer(current[micro_at], norm_gain[layer_at], w_qkv[layer_at], w_out[layer_at], cache_keys[layer_at, micro_at], cache_values[layer_at, micro_at], cache_lengths[micro_at]))
        current = jnp.stack(produced)
        collected.append(current)
    return jnp.stack(collected)
```

```python
import functools
import math

import jax
import jax.numpy as jnp
from jax import lax
from jax.experimental import pallas as pl
from jax.experimental.pallas import tpu as pltpu
from jax.sharding import PartitionSpec as P

D = 4096
HEADS = 32
KVH = 8
MESH = pl.DeviceIdType.MESH


def far_first(n):
    order = []
    for k in range(n // 2, 0, -1):
        order.append(k)
        if n - k != k:
            order.append(n - k)
    return order


def kernel(
    sizes,
    lens_ref,
    hidden_ref,
    gain_ref,
    wq_hbm,
    wo_hbm,
    keys_hbm,
    vals_hbm,
    out_ref,
    wq,
    wo,
    keys,
    vals,
    cos8,
    sin8,
    state,
    prev,
    pin,
    rs_out,
    rs_in,
    att,
    po,
    load_sem,
    rs_send,
    rs_recv,
    att_send,
    att_recv,
    po_send,
    po_recv,
    prev_send,
    prev_recv,
    out_send,
    out_recv,
):
    n_sec, n_row, n_col = sizes
    s = lax.axis_index("section")
    r = lax.axis_index("row")
    c = lax.axis_index("col")
    last = n_sec - 1
    micro, batch, feats = state.shape
    seqs = batch // n_col
    hd = keys.shape[-1]
    length = keys.shape[2]
    width = wq.shape[1]
    per_group = HEADS // KVH
    rows8 = per_group * seqs

    def at(sec, row, col):
        return {"section": sec, "row": row, "col": col}

    loads = [
        pltpu.make_async_copy(wq_hbm, wq, load_sem.at[0]),
        pltpu.make_async_copy(wo_hbm, wo, load_sem.at[1]),
        pltpu.make_async_copy(keys_hbm, keys, load_sem.at[2]),
        pltpu.make_async_copy(vals_hbm, vals, load_sem.at[3]),
    ]
    for load in loads:
        load.start()

    barrier = pltpu.get_barrier_semaphore()

    def greet(device):
        pl.semaphore_signal(barrier, inc=1, device_id=device, device_id_type=MESH)

    for j in far_first(n_col):
        greet(at(s, r, lax.rem(c + j, n_col)))

    @pl.when(s < last)
    def _():
        for j in range(n_row):
            greet(at(s + 1, lax.rem(r + j, n_row), c))

    @pl.when(s > 0)
    def _():
        for j in range(n_row):
            greet(at(s - 1, lax.rem(r + j, n_row), c))

    @pl.when(s == last)
    def _():
        for j in range(1, n_row):
            greet(at(s, lax.rem(r + j, n_row), c))

    lane = lax.broadcasted_iota(jnp.int32, (rows8, hd), 1)
    row8 = lax.broadcasted_iota(jnp.int32, (rows8, hd), 0)
    half = lax.rem(lane, hd // 2).astype(jnp.float32)
    inverse_freq = jnp.exp(half * (-2.0 / hd * math.log(500000.0)))
    sign = jnp.where(lane < hd // 2, -1.0, 1.0)

    def lengths_of(m):
        value = jnp.full((rows8, hd), lens_ref[m * seqs], jnp.int32)
        for b in range(1, seqs):
            value = jnp.where(lax.rem(row8, seqs) == b, lens_ref[m * seqs + b], value)
        return value

    for m in range(micro):
        angle = lengths_of(m).astype(jnp.float32) * inverse_freq
        cos8[m] = jnp.cos(angle)
        sin8[m] = jnp.sin(angle) * sign

    loads[0].wait()
    pl.semaphore_wait(
        barrier,
        n_col
        - 1
        + jnp.where(s < last, n_row, 0)
        + jnp.where(s > 0, n_row, 0)
        + jnp.where(s == last, n_row - 1, 0),
    )

    def summed(region, m, base):
        total = pin[region, m, 0].astype(jnp.float32)
        for k in range(1, n_row):
            total = total + pin[region, m, k].astype(jnp.float32)
        return (base.astype(jnp.float32) + total).astype(jnp.bfloat16)

    gain = gain_ref[...].astype(jnp.float32)

    def stage_a(m, carry):
        @pl.when(s == 0)
        def _():
            state[m] = hidden_ref[m]

        @pl.when(s > 0)
        def _():
            pltpu.make_async_copy(prev.at[m], prev.at[m], prev_recv.at[m]).wait()
            pltpu.make_async_copy(pin.at[0, m], pin.at[0, m], po_recv.at[0, m]).wait()
            state[m] = summed(0, m, prev[m])

        h_float = state[m].astype(jnp.float32)
        scaled = (h_float * gain).astype(jnp.bfloat16)
        partial = jnp.dot(scaled, wq[...], preferred_element_type=jnp.float32)
        squares = jnp.sum(h_float * h_float, axis=1, keepdims=True)
        squares = jnp.broadcast_to(squares, (batch, hd))
        for k in range(n_col):
            rs_out[m, k, :, 0:width] = partial[k * seqs : (k + 1) * seqs]
            rs_out[m, k, :, width : width + hd] = squares[k * seqs : (k + 1) * seqs]
        for j in far_first(n_col):
            to = lax.rem(c + j, n_col)
            pltpu.make_async_remote_copy(
                src_ref=rs_out.at[m, to],
                dst_ref=rs_in.at[m, j - 1],
                send_sem=rs_send.at[m],
                recv_sem=rs_recv.at[m],
                device_id=at(s, r, to),
                device_id_type=MESH,
            ).start()

        @pl.when(s < last)
        def _():
            pltpu.make_async_remote_copy(
                src_ref=state.at[m],
                dst_ref=prev.at[m],
                send_sem=prev_send.at[m],
                recv_sem=prev_recv.at[m],
                device_id=at(s + 1, r, c),
                device_id_type=MESH,
            ).start()

        @pl.when(s > 0)
        def _():
            pltpu.make_async_remote_copy(
                src_ref=state.at[m],
                dst_ref=out_ref.at[m],
                send_sem=out_send.at[m],
                recv_sem=out_recv.at[m],
                device_id=at(s - 1, r, c),
                device_id_type=MESH,
            ).start()

        return carry

    lax.fori_loop(0, micro, stage_a, 0)

    loads[2].wait()
    loads[3].wait()
    score_scale = 1.0 / math.sqrt(hd)

    def stage_b(m, carry):
        pltpu.make_async_copy(rs_in.at[m], rs_in.at[m], rs_recv.at[m]).wait()
        total = rs_out[m, c]
        for j in range(n_col - 1):
            total = total + rs_in[m, j]
        factor = lax.rsqrt(total[:, width : width + hd] / D + 1e-05)
        heads = [total[:, h * hd : (h + 1) * hd] * factor for h in range(per_group + 2)]
        cos = cos8[m]
        sin = sin8[m]

        def rotate(x):
            return (x * cos + pltpu.roll(x, hd // 2, 1) * sin).astype(jnp.bfloat16)

        queries = rotate(jnp.concatenate(heads[:per_group], axis=0))
        new_key = rotate(jnp.concatenate([heads[per_group]] * per_group, axis=0))
        new_value = jnp.concatenate([heads[per_group + 1]] * per_group, axis=0)
        new_value = new_value.astype(jnp.bfloat16).astype(jnp.float32)
        which = lax.rem(row8, seqs)
        scores = None
        for b in range(seqs):
            mine = lax.dot_general(
                queries,
                keys[m, b],
                (((1,), (1,)), ((), ())),
                preferred_element_type=jnp.float32,
            )
            scores = mine if b == 0 else jnp.where(which == b, mine, scores)
        scores = scores * score_scale
        own = queries.astype(jnp.float32) * new_key.astype(jnp.float32)
        own = jnp.sum(own, axis=1, keepdims=True) * score_scale
        scores = jnp.where(lane < lengths_of(m), scores, -jnp.inf)
        top = jnp.maximum(jnp.max(scores, axis=1, keepdims=True), own)
        cache_exp = jnp.exp(scores - top)
        own_exp = jnp.exp(own - top)
        denom = jnp.sum(cache_exp, axis=1, keepdims=True) + own_exp
        weight = (cache_exp / denom).astype(jnp.bfloat16)
        own_weight = (own_exp / denom).astype(jnp.bfloat16).astype(jnp.float32)
        result = None
        for b in range(seqs):
            mine = jnp.dot(weight, vals[m, b], preferred_element_type=jnp.float32)
            result = mine if b == 0 else jnp.where(which == b, mine, result)
        result = (result + own_weight * new_value).astype(jnp.bfloat16)
        for h in range(per_group):
            att[m, c, :, h * hd : (h + 1) * hd] = result[h * seqs : (h + 1) * seqs]
        for j in far_first(n_col):
            pltpu.make_async_remote_copy(
                src_ref=att.at[m, c],
                dst_ref=att.at[m, c],
                send_sem=att_send.at[m],
                recv_sem=att_recv.at[m],
                device_id=at(s, r, lax.rem(c + j, n_col)),
                device_id_type=MESH,
            ).start()
        return carry

    lax.fori_loop(0, micro, stage_b, 0)

    loads[1].wait()
    region = jnp.where(s == last, 1, 0)
    target = jnp.where(s == last, last, s + 1)

    def stage_c(m, carry):
        others = att.at[m, pl.ds(0, n_col - 1)]
        pltpu.make_async_copy(others, others, att_recv.at[m]).wait()
        rows = jnp.concatenate([att[m, k] for k in range(n_col)], axis=0)
        mixed = jnp.dot(rows, wo[...], preferred_element_type=jnp.float32).astype(jnp.bfloat16)
        po[m] = mixed

        @pl.when(s == last)
        def _():
            pin[1, m, r] = mixed

        def send(j):
            pltpu.make_async_remote_copy(
                src_ref=po.at[m],
                dst_ref=pin.at[region, m, r],
                send_sem=po_send.at[m],
                recv_sem=po_recv.at[region, m],
                device_id=at(target, lax.rem(r + j, n_row), c),
                device_id_type=MESH,
            ).start()

        for j in far_first(n_row):
            send(j)

        @pl.when(s < last)
        def _():
            send(0)

        return carry

    lax.fori_loop(0, micro, stage_c, 0)

    def finish(m, carry):
        @pl.when(s == last)
        def _():
            others = pin.at[1, m, pl.ds(0, n_row - 1)]
            pltpu.make_async_copy(others, others, po_recv.at[1, m]).wait()
            out_ref[m] = summed(1, m, state[m])
            pltpu.make_async_copy(others, others, po_send.at[m]).wait()

        @pl.when(s < last)
        def _():
            pltpu.make_async_copy(out_ref.at[m], out_ref.at[m], out_recv.at[m]).wait()
            pltpu.make_async_copy(state.at[m], state.at[m], prev_send.at[m]).wait()
            pltpu.make_async_copy(pin.at[0, m], pin.at[0, m], po_send.at[m]).wait()

        @pl.when(s > 0)
        def _():
            pltpu.make_async_copy(state.at[m], state.at[m], out_send.at[m]).wait()

        pltpu.make_async_copy(rs_in.at[m], rs_in.at[m], rs_send.at[m]).wait()
        others = att.at[m, pl.ds(0, n_col - 1)]
        pltpu.make_async_copy(others, others, att_send.at[m]).wait()
        return carry

    lax.fori_loop(0, micro, finish, 0)


def solution(mesh):
    n_sec, n_row, n_col = mesh.shape["section"], mesh.shape["row"], mesh.shape["col"]

    def shards(hidden, norm_gain, w_qkv, w_out, cache_keys, cache_values, cache_lengths):
        micro, batch, feats = hidden.shape
        wq = w_qkv[0]
        wo = w_out[0]
        width = wq.shape[1]
        _, _, seqs, length, groups, hd = cache_keys.shape
        keys = cache_keys.reshape(micro, seqs, length, hd)
        vals = cache_values.reshape(micro, seqs, length, hd)
        rows8 = HEADS // KVH * seqs
        bf, f32 = jnp.bfloat16, jnp.float32
        vmem = pl.BlockSpec(memory_space=pltpu.VMEM)
        hbm = pl.BlockSpec(memory_space=pl.ANY)
        sem = pltpu.SemaphoreType.DMA
        out = pl.pallas_call(
            functools.partial(kernel, (n_sec, n_row, n_col)),
            out_shape=jax.ShapeDtypeStruct((micro, batch, feats), bf),
            in_specs=[pl.BlockSpec(memory_space=pltpu.SMEM), vmem, vmem, hbm, hbm, hbm, hbm],
            out_specs=vmem,
            scratch_shapes=[
                pltpu.VMEM(wq.shape, bf),
                pltpu.VMEM(wo.shape, bf),
                pltpu.VMEM(keys.shape, bf),
                pltpu.VMEM(vals.shape, bf),
                pltpu.VMEM((micro, rows8, hd), f32),
                pltpu.VMEM((micro, rows8, hd), f32),
                pltpu.VMEM((micro, batch, feats), bf),
                pltpu.VMEM((micro, batch, feats), bf),
                pltpu.VMEM((2, micro, n_row, batch, feats), bf),
                pltpu.VMEM((micro, n_col, seqs, width + hd), f32),
                pltpu.VMEM((micro, n_col - 1, seqs, width + hd), f32),
                pltpu.VMEM((micro, n_col, seqs, wo.shape[0]), bf),
                pltpu.VMEM((micro, batch, feats), bf),
                sem((4,)),
                sem((micro,)),
                sem((micro,)),
                sem((micro,)),
                sem((micro,)),
                sem((micro,)),
                sem((2, micro)),
                sem((micro,)),
                sem((micro,)),
                sem((micro,)),
                sem((micro,)),
            ],
            compiler_params=pltpu.CompilerParams(collective_id=0, has_side_effects=True),
        )(cache_lengths.reshape(-1), hidden, norm_gain, wq, wo, keys, vals)
        return out[None]

    return jax.shard_map(
        shards,
        mesh=mesh,
        in_specs=(
            P(None, None, "col"),
            P("section", "col"),
            P("section", "col", "row"),
            P("section", "row", "col"),
            P("section", None, "col", None, "row", None),
            P("section", None, "col", None, "row", None),
            P(None, "col"),
        ),
        out_specs=P("section", None, None, "col"),
        check_vma=False,
    )
```

```python
import functools
import math

import jax
import jax.numpy as jnp
from jax import lax
from jax.experimental import pallas as pl
from jax.experimental.pallas import tpu as pltpu
from jax.sharding import PartitionSpec as P

D = 4096
HEADS = 32
KVH = 8
MESH = pl.DeviceIdType.MESH
BY_SEQUENCE = (1, 3, 4, 6)
CHUNKS = 4


def far_first(n):
    order = []
    for k in range(n // 2, 0, -1):
        order.append(k)
        if n - k != k:
            order.append(n - k)
    return order


def one_of(value, choices):
    hit = value < 0
    for choice in choices:
        hit = hit | (value == choice)
    return hit


def rows_of(ref, index, count):
    return jnp.concatenate([ref[index, k] for k in range(count)], axis=0)


def kernel(
    sizes,
    lens_ref,
    hidden_ref,
    gain_ref,
    wq_hbm,
    wo_hbm,
    keys_hbm,
    vals_hbm,
    out_ref,
    wq,
    wo,
    keys,
    vals,
    cos8,
    sin8,
    gains,
    gain32,
    rows,
    state,
    prev,
    given,
    pin,
    rs_out,
    rs_in,
    total,
    att,
    po,
    load_sem,
    wq_send,
    wq_recv,
    wo_send,
    wo_recv,
    gain_send,
    gain_recv,
    go_sem,
    rs_send,
    rs_recv,
    att_send,
    att_recv,
    po_send,
    po_recv,
    prev_send,
    prev_recv,
    out_send,
    out_recv,
):
    n_sec, n_row, n_col = sizes
    s = lax.axis_index("section")
    r = lax.axis_index("row")
    c = lax.axis_index("col")
    last = n_sec - 1
    micro, n_blocks, seqs, feats = state.shape
    batch = n_col * seqs
    hd = keys.shape[-1]
    width = wq.shape[1]
    per_group = HEADS // KVH
    rows8 = per_group * seqs
    out_seq = one_of(s, BY_SEQUENCE)
    out_feat = jnp.logical_not(out_seq)
    in_seq = one_of(s, [b + 1 for b in BY_SEQUENCE])
    in_feat = jnp.logical_not(in_seq)
    right, left = lax.rem(c + 1, n_col), lax.rem(c + n_col - 1, n_col)

    def at(sec, row, col):
        return {"section": sec, "row": row, "col": col}

    my_rows = pl.ds(pl.multiple_of(c * feats, feats), feats)
    load_wq = pltpu.make_async_copy(wq_hbm, wq.at[my_rows], load_sem.at[0])
    load_wo = pltpu.make_async_copy(wo_hbm, wo.at[c], load_sem.at[1])
    load_keys = pltpu.make_async_copy(keys_hbm, keys, load_sem.at[2])
    load_vals = pltpu.make_async_copy(vals_hbm, vals, load_sem.at[3])
    load_wq.start()
    load_wo.start()
    load_keys.start()
    load_vals.start()

    barrier = pltpu.get_barrier_semaphore()

    def greet(device):
        pl.semaphore_signal(barrier, inc=1, device_id=device, device_id_type=MESH)

    for j in far_first(n_col):
        greet(at(s, r, lax.rem(c + j, n_col)))

    @pl.when(s < last)
    def _():
        for j in range(n_row):
            greet(at(s + 1, lax.rem(r + j, n_row), c))
        for j in range(1, n_col):
            greet(at(s + 1, r, lax.rem(c + j, n_col)))

    @pl.when(s > 0)
    def _():
        for j in range(n_row):
            greet(at(s - 1, lax.rem(r + j, n_row), c))
        for j in range(1, n_col):
            greet(at(s - 1, r, lax.rem(c + j, n_col)))

    @pl.when(s == last)
    def _():
        for j in range(1, n_row):
            greet(at(s, lax.rem(r + j, n_row), c))

    lane = lax.broadcasted_iota(jnp.int32, (rows8, hd), 1)
    row8 = lax.broadcasted_iota(jnp.int32, (rows8, hd), 0)
    half = lax.rem(lane, hd // 2).astype(jnp.float32)
    inverse_freq = jnp.exp(half * (-2.0 / hd * math.log(500000.0)))
    sign = jnp.where(lane < hd // 2, -1.0, 1.0)

    def lengths_of(m):
        value = jnp.full((rows8, hd), lens_ref[m * seqs], jnp.int32)
        for b in range(1, seqs):
            value = jnp.where(lax.rem(row8, seqs) == b, lens_ref[m * seqs + b], value)
        return value

    for m in range(micro):
        angle = lengths_of(m).astype(jnp.float32) * inverse_freq
        cos8[m] = jnp.cos(angle)
        sin8[m] = jnp.sin(angle) * sign
    gain32[...] = jnp.broadcast_to(gain_ref[...].astype(jnp.float32), gain32.shape)
    gains[c] = gain_ref[...]

    load_wq.wait()
    load_wo.wait()
    across = n_row + n_col - 1
    pl.semaphore_wait(
        barrier,
        n_col
        - 1
        + jnp.where(s < last, across, 0)
        + jnp.where(s > 0, across, 0)
        + jnp.where(s == last, n_row - 1, 0),
    )

    def gather(part, send_sem, recv_sem):
        def copy(way, step, block, piece, to):
            return pltpu.make_async_remote_copy(
                src_ref=part(block, piece),
                dst_ref=part(block, piece),
                send_sem=send_sem,
                recv_sem=recv_sem.at[way, step, piece],
                device_id=at(s, r, to),
                device_id_type=MESH,
            )

        def arrived(way, step, piece):
            pltpu.make_async_copy(part(0, 0), part(0, 0), recv_sem.at[way, step, piece]).wait()

        for piece in range(CHUNKS):
            copy(0, 0, c, piece, right).start()
            copy(1, 0, c, piece, left).start()

        rightward, leftward = n_col // 2, n_col - 1 - n_col // 2

        def forward(step, carry):
            for piece in range(CHUNKS):
                arrived(0, step - 1, piece)
                copy(0, step, lax.rem(c + n_col - step, n_col), piece, right).start()

                @pl.when(step < leftward)
                def _():
                    arrived(1, step - 1, piece)
                    copy(1, step, lax.rem(c + step, n_col), piece, left).start()

            return carry

        lax.fori_loop(1, rightward, forward, 0)
        for piece in range(CHUNKS):
            arrived(0, rightward - 1, piece)
            arrived(1, leftward - 1, piece)

        def sent(k, carry):
            for piece in range(CHUNKS):
                pltpu.make_async_copy(part(0, 0), part(0, 0), send_sem).wait()
            return carry

        lax.fori_loop(0, n_col - 1, sent, 0)

    piece_rows = feats // CHUNKS

    def wq_part(block, piece):
        first = pl.multiple_of(block * feats + piece * piece_rows, piece_rows)
        return wq.at[pl.ds(first, piece_rows)]

    wo_rows = wo.shape[1] // CHUNKS

    def wo_part(block, piece):
        return wo.at[block, pl.ds(piece * wo_rows, wo_rows)]

    odd = lax.rem(s, 2) == 1

    @pl.when(odd & (s > 1))
    def _():
        pl.semaphore_wait(go_sem, 1)

    @pl.when(in_seq)
    def _():
        for j in far_first(n_col):
            pltpu.make_async_remote_copy(
                src_ref=gains.at[c],
                dst_ref=gains.at[c],
                send_sem=gain_send,
                recv_sem=gain_recv,
                device_id=at(s, r, lax.rem(c + j, n_col)),
                device_id_type=MESH,
            ).start()
        gather(wq_part, wq_send, wq_recv)
        others = gains.at[pl.ds(0, n_col - 1)]
        pltpu.make_async_copy(others, others, gain_recv).wait()
        pltpu.make_async_copy(others, others, gain_send).wait()
        for k in range(n_col):
            gain32[k * seqs : (k + 1) * seqs] = jnp.broadcast_to(
                gains[k].astype(jnp.float32), (seqs, feats)
            )

    @pl.when(out_seq)
    def _():
        gather(wo_part, wo_send, wo_recv)

    @pl.when(jnp.logical_not(odd) & (s > 0))
    def _():
        pl.semaphore_signal(go_sem, inc=1, device_id=at(s + 1, r, c), device_id_type=MESH)

    load_keys.wait()
    load_vals.wait()
    score_scale = 1.0 / math.sqrt(hd)

    def summed(region, m, base):
        mixed = pin[region, m, 0].astype(jnp.float32)
        for k in range(1, n_row):
            mixed = mixed + pin[region, m, k].astype(jnp.float32)
        return (base.astype(jnp.float32) + mixed).astype(jnp.bfloat16)

    def hand_over(m, to_section, buffer, same, send_sem, recv_sem):
        @pl.when(same)
        def _():
            pltpu.make_async_remote_copy(
                src_ref=state.at[m],
                dst_ref=buffer.at[m],
                send_sem=send_sem.at[m],
                recv_sem=recv_sem.at[m],
                device_id=at(to_section, r, c),
                device_id_type=MESH,
            ).start()

        @pl.when(jnp.logical_not(same))
        def _():
            for j in [*far_first(n_col), 0]:
                to = lax.rem(c + j, n_col)
                pltpu.make_async_remote_copy(
                    src_ref=state.at[m, to],
                    dst_ref=buffer.at[m, c],
                    send_sem=send_sem.at[m],
                    recv_sem=recv_sem.at[m],
                    device_id=at(to_section, r, to),
                    device_id_type=MESH,
                ).start()

    def take_state(m):
        @pl.when(s == 0)
        def _():
            rows[m] = hidden_ref[m]

        @pl.when(s > 0)
        def _():
            pltpu.make_async_copy(prev.at[m], prev.at[m], prev_recv.at[m]).wait()
            base = rows_of(prev, m, n_blocks)
            pltpu.make_async_copy(pin.at[0, m], pin.at[0, m], po_recv.at[0, m]).wait()
            rows[m] = summed(0, m, base)

        return rows[m]

    def pass_on(m):
        value = rows[m]
        for k in range(n_blocks):
            state[m, k] = value[k * seqs : (k + 1) * seqs]

        @pl.when(s < last)
        def _():
            hand_over(m, s + 1, prev, in_seq == out_seq, prev_send, prev_recv)

        @pl.when(s > 0)
        def _():
            hand_over(m, s - 1, given, in_feat, out_send, out_recv)

        @pl.when((s == last) & in_seq)
        def _():
            given[m, c] = state[m, c]
            for j in far_first(n_col):
                to = lax.rem(c + j, n_col)
                pltpu.make_async_remote_copy(
                    src_ref=state.at[m, to],
                    dst_ref=given.at[m, c],
                    send_sem=prev_send.at[m],
                    recv_sem=out_recv.at[m],
                    device_id=at(s, r, to),
                    device_id_type=MESH,
                ).start()

    def scale(value):
        h_float = value.astype(jnp.float32)
        return h_float * h_float, (h_float * gain32[...]).astype(jnp.bfloat16)

    def project_features(m, carry):
        value = take_state(m)
        squares, scaled = scale(value)
        own_rows = pl.ds(pl.multiple_of(c * feats, feats), feats)
        partial = jnp.dot(scaled, wq[own_rows, :], preferred_element_type=jnp.float32)
        squares = jnp.sum(squares, axis=1, keepdims=True)
        squares = jnp.broadcast_to(squares, (batch, hd))
        for k in range(n_col):
            rs_out[m, k, :, 0:width] = partial[k * seqs : (k + 1) * seqs]
            rs_out[m, k, :, width : width + hd] = squares[k * seqs : (k + 1) * seqs]
        for j in far_first(n_col):
            to = lax.rem(c + j, n_col)
            pltpu.make_async_remote_copy(
                src_ref=rs_out.at[m, to],
                dst_ref=rs_in.at[m, j - 1],
                send_sem=rs_send.at[m],
                recv_sem=rs_recv.at[m],
                device_id=at(s, r, to),
                device_id_type=MESH,
            ).start()
        pass_on(m)
        return carry

    @pl.when(in_feat)
    def _():
        lax.fori_loop(0, micro, project_features, 0)

    region = jnp.where(s == last, 1, 0)
    target = jnp.where(s == last, last, s + 1)

    def send_rows(m):
        def send(j):
            pltpu.make_async_remote_copy(
                src_ref=po.at[m],
                dst_ref=pin.at[region, m, r],
                send_sem=po_send.at[m],
                recv_sem=po_recv.at[region, m],
                device_id=at(target, lax.rem(r + j, n_row), c),
                device_id_type=MESH,
            ).start()

        for j in far_first(n_row):
            send(j)

        @pl.when(s < last)
        def _():
            send(0)

    def attend(m):
        factor = lax.rsqrt(total[:, width : width + hd] / D + 1e-05)
        heads = [total[:, h * hd : (h + 1) * hd] * factor for h in range(per_group + 2)]
        cos = cos8[m]
        sin = sin8[m]

        def rotate(x):
            return (x * cos + pltpu.roll(x, hd // 2, 1) * sin).astype(jnp.bfloat16)

        queries = rotate(jnp.concatenate(heads[:per_group], axis=0))
        new_key = rotate(jnp.concatenate([heads[per_group]] * per_group, axis=0))
        new_value = jnp.concatenate([heads[per_group + 1]] * per_group, axis=0)
        new_value = new_value.astype(jnp.bfloat16).astype(jnp.float32)
        which = lax.rem(row8, seqs)
        scores = None
        for b in range(seqs):
            mine = lax.dot_general(
                queries,
                keys[m, b],
                (((1,), (1,)), ((), ())),
                preferred_element_type=jnp.float32,
            )
            scores = mine if b == 0 else jnp.where(which == b, mine, scores)
        scores = scores * score_scale
        own = queries.astype(jnp.float32) * new_key.astype(jnp.float32)
        own = jnp.sum(own, axis=1, keepdims=True) * score_scale
        scores = jnp.where(lane < lengths_of(m), scores, -jnp.inf)
        top = jnp.maximum(jnp.max(scores, axis=1, keepdims=True), own)
        cache_exp = jnp.exp(scores - top)
        own_exp = jnp.exp(own - top)
        denom = jnp.sum(cache_exp, axis=1, keepdims=True) + own_exp
        weight = (cache_exp / denom).astype(jnp.bfloat16)
        own_weight = (own_exp / denom).astype(jnp.bfloat16).astype(jnp.float32)
        result = None
        for b in range(seqs):
            mine = jnp.dot(weight, vals[m, b], preferred_element_type=jnp.float32)
            result = mine if b == 0 else jnp.where(which == b, mine, result)
        return (result + own_weight * new_value).astype(jnp.bfloat16)

    def middle(m, carry):
        @pl.when(in_feat)
        def _():
            pltpu.make_async_copy(rs_in.at[m], rs_in.at[m], rs_recv.at[m]).wait()
            whole = rs_out[m, c]
            for j in range(n_col - 1):
                whole = whole + rs_in[m, j]
            total[...] = whole

        @pl.when(in_seq)
        def _():
            value = take_state(m)
            squares, scaled = scale(value)
            across = jnp.concatenate(
                [scaled[k * seqs : (k + 1) * seqs] for k in range(n_blocks)], axis=1
            )
            total[:, 0:width] = jnp.dot(across, wq[...], preferred_element_type=jnp.float32)
            both = squares[0:seqs]
            for k in range(1, n_blocks):
                both = both + squares[k * seqs : (k + 1) * seqs]
            both = jnp.sum(both, axis=1, keepdims=True)
            total[:, width : width + hd] = jnp.broadcast_to(both, (seqs, hd))

        result = attend(m)

        @pl.when(out_feat)
        def _():
            for h in range(per_group):
                att[m, c, :, h * hd : (h + 1) * hd] = result[h * seqs : (h + 1) * seqs]
            for j in far_first(n_col):
                pltpu.make_async_remote_copy(
                    src_ref=att.at[m, c],
                    dst_ref=att.at[m, c],
                    send_sem=att_send.at[m],
                    recv_sem=att_recv.at[m],
                    device_id=at(s, r, lax.rem(c + j, n_col)),
                    device_id_type=MESH,
                ).start()

        @pl.when(out_seq)
        def _():
            flat = jnp.concatenate(
                [result[h * seqs : (h + 1) * seqs] for h in range(per_group)], axis=1
            )
            for k in range(n_blocks):
                mixed = jnp.dot(flat, wo[k], preferred_element_type=jnp.float32)
                po[m, k * seqs : (k + 1) * seqs] = mixed.astype(jnp.bfloat16)
            send_rows(m)

        @pl.when(in_seq)
        def _():
            pass_on(m)

        return carry

    lax.fori_loop(0, micro, middle, 0)

    def mix_features(m, carry):
        others = att.at[m, pl.ds(0, n_col - 1)]
        pltpu.make_async_copy(others, others, att_recv.at[m]).wait()
        mixed = jnp.dot(rows_of(att, m, n_col), wo[c], preferred_element_type=jnp.float32)
        mixed = mixed.astype(jnp.bfloat16)
        po[m] = mixed

        @pl.when(s == last)
        def _():
            pin[1, m, r] = mixed

        send_rows(m)
        pltpu.make_async_copy(others, others, att_send.at[m]).wait()
        return carry

    @pl.when(out_feat)
    def _():
        lax.fori_loop(0, micro, mix_features, 0)

    def finish(m, carry):
        @pl.when(s == last)
        def _():
            others = pin.at[1, m, pl.ds(0, n_row - 1)]
            pltpu.make_async_copy(others, others, po_recv.at[1, m]).wait()
            if last - 1 in BY_SEQUENCE:
                blocks = given.at[m, pl.ds(0, n_col - 1)]
                pltpu.make_async_copy(blocks, blocks, out_recv.at[m]).wait()
                pltpu.make_async_copy(blocks, blocks, prev_send.at[m]).wait()
                base = rows_of(given, m, n_blocks)
            else:
                base = rows[m]
            out_ref[m] = summed(1, m, base)
            pltpu.make_async_copy(others, others, po_send.at[m]).wait()

        @pl.when(s < last)
        def _():
            pltpu.make_async_copy(given.at[m], given.at[m], out_recv.at[m]).wait()
            out_ref[m] = rows_of(given, m, n_blocks)
            pltpu.make_async_copy(state.at[m], state.at[m], prev_send.at[m]).wait()
            pltpu.make_async_copy(pin.at[0, m], pin.at[0, m], po_send.at[m]).wait()

        @pl.when(s > 0)
        def _():
            pltpu.make_async_copy(state.at[m], state.at[m], out_send.at[m]).wait()

        @pl.when(in_feat)
        def _():
            pltpu.make_async_copy(rs_in.at[m], rs_in.at[m], rs_send.at[m]).wait()

        return carry

    lax.fori_loop(0, micro, finish, 0)


def solution(mesh):
    n_sec, n_row, n_col = mesh.shape["section"], mesh.shape["row"], mesh.shape["col"]

    def shards(hidden, norm_gain, w_qkv, w_out, cache_keys, cache_values, cache_lengths):
        micro, batch, feats = hidden.shape
        wq = w_qkv[0]
        wo = w_out[0]
        width = wq.shape[1]
        _, _, seqs, length, groups, hd = cache_keys.shape
        keys = cache_keys.reshape(micro, seqs, length, hd)
        vals = cache_values.reshape(micro, seqs, length, hd)
        rows8 = HEADS // KVH * seqs
        bf, f32 = jnp.bfloat16, jnp.float32
        vmem = pl.BlockSpec(memory_space=pltpu.VMEM)
        hbm = pl.BlockSpec(memory_space=pl.ANY)
        sem = pltpu.SemaphoreType.DMA
        out = pl.pallas_call(
            functools.partial(kernel, (n_sec, n_row, n_col)),
            out_shape=jax.ShapeDtypeStruct((micro, batch, feats), bf),
            in_specs=[pl.BlockSpec(memory_space=pltpu.SMEM), vmem, vmem, hbm, hbm, hbm, hbm],
            out_specs=vmem,
            scratch_shapes=[
                pltpu.VMEM((n_col * feats, width), bf),
                pltpu.VMEM((n_col, *wo.shape), bf),
                pltpu.VMEM(keys.shape, bf),
                pltpu.VMEM(vals.shape, bf),
                pltpu.VMEM((micro, rows8, hd), f32),
                pltpu.VMEM((micro, rows8, hd), f32),
                pltpu.VMEM((n_col, 1, feats), bf),
                pltpu.VMEM((batch, feats), f32),
                pltpu.VMEM((micro, batch, feats), bf),
                pltpu.VMEM((micro, n_col, seqs, feats), bf),
                pltpu.VMEM((micro, n_col, seqs, feats), bf),
                pltpu.VMEM((micro, n_col, seqs, feats), bf),
                pltpu.VMEM((2, micro, n_row, batch, feats), bf),
                pltpu.VMEM((micro, n_col, seqs, width + hd), f32),
                pltpu.VMEM((micro, n_col - 1, seqs, width + hd), f32),
                pltpu.VMEM((seqs, width + hd), f32),
                pltpu.VMEM((micro, n_col, seqs, wo.shape[0]), bf),
                pltpu.VMEM((micro, batch, feats), bf),
                sem((4,)),
                sem,
                sem((2, n_col // 2, CHUNKS)),
                sem,
                sem((2, n_col // 2, CHUNKS)),
                sem,
                sem,
                pltpu.SemaphoreType.REGULAR,
                sem((micro,)),
                sem((micro,)),
                sem((micro,)),
                sem((micro,)),
                sem((micro,)),
                sem((2, micro)),
                sem((micro,)),
                sem((micro,)),
                sem((micro,)),
                sem((micro,)),
            ],
            compiler_params=pltpu.CompilerParams(
                collective_id=0, has_side_effects=True, vmem_limit_bytes=48 << 20
            ),
        )(cache_lengths.reshape(-1), hidden, norm_gain, wq, wo, keys, vals)
        return out[None]

    return jax.shard_map(
        shards,
        mesh=mesh,
        in_specs=(
            P(None, None, "col"),
            P("section", "col"),
            P("section", "col", "row"),
            P("section", "row", "col"),
            P("section", None, "col", None, "row", None),
            P("section", None, "col", None, "row", None),
            P(None, "col"),
        ),
        out_specs=P("section", None, None, "col"),
        check_vma=False,
    )
```

```python
import functools
import math

import jax
import jax.numpy as jnp
from jax import lax
from jax.experimental import pallas as pl
from jax.experimental.pallas import tpu as pltpu
from jax.sharding import PartitionSpec as P

D = 4096
HEADS = 32
KVH = 8
MESH = pl.DeviceIdType.MESH
BY_SEQUENCE = (3, 5, 6)
CHUNKS = 4


def far_first(n):
    order = []
    for k in range(n // 2, 0, -1):
        order.append(k)
        if n - k != k:
            order.append(n - k)
    return order


def one_of(value, choices):
    hit = value < 0
    for choice in choices:
        hit = hit | (value == choice)
    return hit


def rows_of(ref, index, count):
    return jnp.concatenate([ref[index, k] for k in range(count)], axis=0)


def kernel(
    sizes,
    lens_hbm,
    hidden_hbm,
    gain_hbm,
    wq_hbm,
    wo_hbm,
    keys_hbm,
    vals_hbm,
    out_ref,
    lens_ref,
    hidden_ref,
    gain_ref,
    wq,
    wo,
    keys,
    vals,
    cos8,
    sin8,
    gains,
    gain32,
    rows,
    state,
    prev,
    given,
    pin,
    rs_out,
    rs_in,
    total,
    att,
    po,
    load_sem,
    wq_send,
    wq_recv,
    wo_send,
    wo_recv,
    gain_send,
    gain_recv,
    go_sem,
    rs_send,
    rs_recv,
    att_send,
    att_recv,
    po_send,
    po_recv,
    prev_send,
    prev_recv,
    out_send,
    out_recv,
):
    n_sec, n_row, n_col = sizes
    s = lax.axis_index("section")
    r = lax.axis_index("row")
    c = lax.axis_index("col")
    last = n_sec - 1
    micro, n_blocks, seqs, feats = state.shape
    batch = n_col * seqs
    hd = keys.shape[-1]
    width = wq.shape[1]
    per_group = HEADS // KVH
    rows8 = per_group * seqs
    out_seq = one_of(s, BY_SEQUENCE)
    out_feat = jnp.logical_not(out_seq)
    in_seq = one_of(s, [b + 1 for b in BY_SEQUENCE])
    in_feat = jnp.logical_not(in_seq)
    right, left = lax.rem(c + 1, n_col), lax.rem(c + n_col - 1, n_col)

    def at(sec, row, col):
        return {"section": sec, "row": row, "col": col}

    my_rows = pl.ds(pl.multiple_of(c * feats, feats), feats)
    load_wq = pltpu.make_async_copy(wq_hbm, wq.at[my_rows], load_sem.at[0])
    load_wo = pltpu.make_async_copy(wo_hbm, wo.at[c], load_sem.at[1])
    load_keys = pltpu.make_async_copy(keys_hbm, keys, load_sem.at[2])
    load_vals = pltpu.make_async_copy(vals_hbm, vals, load_sem.at[3])
    load_lens = pltpu.make_async_copy(lens_hbm, lens_ref, load_sem.at[4])
    load_gain = pltpu.make_async_copy(gain_hbm, gain_ref, load_sem.at[5])
    load_hidden = pltpu.make_async_copy(hidden_hbm, hidden_ref, load_sem.at[6])
    load_lens.start()
    load_gain.start()
    load_hidden.start()
    load_wq.start()
    load_wo.start()
    load_keys.start()
    load_vals.start()

    barrier = pltpu.get_barrier_semaphore()

    def greet(device):
        pl.semaphore_signal(barrier, inc=1, device_id=device, device_id_type=MESH)

    for j in far_first(n_col):
        greet(at(s, r, lax.rem(c + j, n_col)))

    @pl.when(s < last)
    def _():
        for j in range(n_row):
            greet(at(s + 1, lax.rem(r + j, n_row), c))
        for j in range(1, n_col):
            greet(at(s + 1, r, lax.rem(c + j, n_col)))

    @pl.when(s > 0)
    def _():
        for j in range(n_row):
            greet(at(s - 1, lax.rem(r + j, n_row), c))
        for j in range(1, n_col):
            greet(at(s - 1, r, lax.rem(c + j, n_col)))

    @pl.when(s == last)
    def _():
        for j in range(1, n_row):
            greet(at(s, lax.rem(r + j, n_row), c))

    load_lens.wait()
    load_gain.wait()
    load_hidden.wait()

    lane = lax.broadcasted_iota(jnp.int32, (rows8, hd), 1)
    row8 = lax.broadcasted_iota(jnp.int32, (rows8, hd), 0)
    half = lax.rem(lane, hd // 2).astype(jnp.float32)
    inverse_freq = jnp.exp(half * (-2.0 / hd * math.log(500000.0)))
    sign = jnp.where(lane < hd // 2, -1.0, 1.0)

    def lengths_of(m):
        value = jnp.full((rows8, hd), lens_ref[0, m], jnp.int32)
        for b in range(1, seqs):
            value = jnp.where(lax.rem(row8, seqs) == b, lens_ref[b, m], value)
        return value

    for m in range(micro):
        angle = lengths_of(m).astype(jnp.float32) * inverse_freq
        cos8[m] = jnp.cos(angle)
        sin8[m] = jnp.sin(angle) * sign
    gain32[...] = jnp.broadcast_to(gain_ref[...].astype(jnp.float32), gain32.shape)
    gains[c] = gain_ref[...]

    load_wq.wait()
    load_wo.wait()
    across = n_row + n_col - 1
    pl.semaphore_wait(
        barrier,
        n_col
        - 1
        + jnp.where(s < last, across, 0)
        + jnp.where(s > 0, across, 0)
        + jnp.where(s == last, n_row - 1, 0),
    )

    def gather(part, send_sem, recv_sem):
        def copy(way, step, block, piece, to):
            return pltpu.make_async_remote_copy(
                src_ref=part(block, piece),
                dst_ref=part(block, piece),
                send_sem=send_sem,
                recv_sem=recv_sem.at[way, step, piece],
                device_id=at(s, r, to),
                device_id_type=MESH,
            )

        def arrived(way, step, piece):
            pltpu.make_async_copy(part(0, 0), part(0, 0), recv_sem.at[way, step, piece]).wait()

        for piece in range(CHUNKS):
            copy(0, 0, c, piece, right).start()
            copy(1, 0, c, piece, left).start()

        steps = n_col // 2

        def forward(step, carry):
            for piece in range(CHUNKS):
                arrived(0, step - 1, piece)

                @pl.when((step < steps - 1) | (piece < CHUNKS // 2))
                def _():
                    copy(0, step, lax.rem(c + n_col - step, n_col), piece, right).start()

                arrived(1, step - 1, piece)

                @pl.when((step < steps - 1) | (piece >= CHUNKS // 2))
                def _():
                    copy(1, step, lax.rem(c + step, n_col), piece, left).start()

            return carry

        lax.fori_loop(1, steps, forward, 0)
        for piece in range(CHUNKS):
            arrived(0 if piece < CHUNKS // 2 else 1, steps - 1, piece)

        def sent(k, carry):
            for piece in range(CHUNKS):
                pltpu.make_async_copy(part(0, 0), part(0, 0), send_sem).wait()
            return carry

        lax.fori_loop(0, n_col - 1, sent, 0)

    piece_rows = feats // CHUNKS

    def wq_part(block, piece):
        first = pl.multiple_of(block * feats + piece * piece_rows, piece_rows)
        return wq.at[pl.ds(first, piece_rows)]

    wo_rows = wo.shape[1] // CHUNKS

    def wo_part(block, piece):
        return wo.at[block, pl.ds(piece * wo_rows, wo_rows)]

    odd = lax.rem(s, 2) == 1

    @pl.when(odd & (s > 1))
    def _():
        pl.semaphore_wait(go_sem, 1)

    @pl.when(in_seq)
    def _():
        for j in far_first(n_col):
            pltpu.make_async_remote_copy(
                src_ref=gains.at[c],
                dst_ref=gains.at[c],
                send_sem=gain_send,
                recv_sem=gain_recv,
                device_id=at(s, r, lax.rem(c + j, n_col)),
                device_id_type=MESH,
            ).start()
        gather(wq_part, wq_send, wq_recv)
        others = gains.at[pl.ds(0, n_col - 1)]
        pltpu.make_async_copy(others, others, gain_recv).wait()
        pltpu.make_async_copy(others, others, gain_send).wait()
        for k in range(n_col):
            gain32[k * seqs : (k + 1) * seqs] = jnp.broadcast_to(
                gains[k].astype(jnp.float32), (seqs, feats)
            )

    @pl.when(out_seq)
    def _():
        gather(wo_part, wo_send, wo_recv)

    @pl.when(jnp.logical_not(odd) & (s > 0))
    def _():
        pl.semaphore_signal(go_sem, inc=1, device_id=at(s + 1, r, c), device_id_type=MESH)

    load_keys.wait()
    load_vals.wait()
    score_scale = 1.0 / math.sqrt(hd)

    def summed(region, m, base):
        mixed = pin[region, m, 0].astype(jnp.float32)
        for k in range(1, n_row):
            mixed = mixed + pin[region, m, k].astype(jnp.float32)
        return (base.astype(jnp.float32) + mixed).astype(jnp.bfloat16)

    def hand_over(m, to_section, buffer, same, send_sem, recv_sem):
        @pl.when(same)
        def _():
            pltpu.make_async_remote_copy(
                src_ref=state.at[m],
                dst_ref=buffer.at[m],
                send_sem=send_sem.at[m],
                recv_sem=recv_sem.at[m],
                device_id=at(to_section, r, c),
                device_id_type=MESH,
            ).start()

        @pl.when(jnp.logical_not(same))
        def _():
            for j in [*far_first(n_col), 0]:
                to = lax.rem(c + j, n_col)
                pltpu.make_async_remote_copy(
                    src_ref=state.at[m, to],
                    dst_ref=buffer.at[m, c],
                    send_sem=send_sem.at[m],
                    recv_sem=recv_sem.at[m],
                    device_id=at(to_section, r, to),
                    device_id_type=MESH,
                ).start()

    def take_state(m):
        @pl.when(s == 0)
        def _():
            rows[m] = hidden_ref[m]

        @pl.when(s > 0)
        def _():
            pltpu.make_async_copy(prev.at[m], prev.at[m], prev_recv.at[m]).wait()
            base = rows_of(prev, m, n_blocks)
            pltpu.make_async_copy(pin.at[0, m], pin.at[0, m], po_recv.at[0, m]).wait()
            rows[m] = summed(0, m, base)

        return rows[m]

    def pass_on(m):
        value = rows[m]
        for k in range(n_blocks):
            state[m, k] = value[k * seqs : (k + 1) * seqs]

        @pl.when(s < last)
        def _():
            hand_over(m, s + 1, prev, in_seq == out_seq, prev_send, prev_recv)

        @pl.when(s > 0)
        def _():
            hand_over(m, s - 1, given, in_feat, out_send, out_recv)

        @pl.when((s == last) & in_seq)
        def _():
            given[m, c] = state[m, c]
            for j in far_first(n_col):
                to = lax.rem(c + j, n_col)
                pltpu.make_async_remote_copy(
                    src_ref=state.at[m, to],
                    dst_ref=given.at[m, c],
                    send_sem=prev_send.at[m],
                    recv_sem=out_recv.at[m],
                    device_id=at(s, r, to),
                    device_id_type=MESH,
                ).start()

    def scale(value):
        h_float = value.astype(jnp.float32)
        return h_float * h_float, (h_float * gain32[...]).astype(jnp.bfloat16)

    def project_features(m):
        value = take_state(m)
        squares, scaled = scale(value)
        own_rows = pl.ds(pl.multiple_of(c * feats, feats), feats)
        partial = jnp.dot(scaled, wq[own_rows, :], preferred_element_type=jnp.float32)
        squares = jnp.sum(squares, axis=1, keepdims=True)
        squares = jnp.broadcast_to(squares, (batch, hd))
        for k in range(n_col):
            rs_out[m, k, :, 0:width] = partial[k * seqs : (k + 1) * seqs]
            rs_out[m, k, :, width : width + hd] = squares[k * seqs : (k + 1) * seqs]
        for j in far_first(n_col):
            to = lax.rem(c + j, n_col)
            pltpu.make_async_remote_copy(
                src_ref=rs_out.at[m, to],
                dst_ref=rs_in.at[m, j - 1],
                send_sem=rs_send.at[m],
                recv_sem=rs_recv.at[m],
                device_id=at(s, r, to),
                device_id_type=MESH,
            ).start()
        pass_on(m)

    region = jnp.where(s == last, 1, 0)
    target = jnp.where(s == last, last, s + 1)

    def send_rows(m):
        def send(j):
            pltpu.make_async_remote_copy(
                src_ref=po.at[m],
                dst_ref=pin.at[region, m, r],
                send_sem=po_send.at[m],
                recv_sem=po_recv.at[region, m],
                device_id=at(target, lax.rem(r + j, n_row), c),
                device_id_type=MESH,
            ).start()

        for j in far_first(n_row):
            send(j)

        @pl.when(s < last)
        def _():
            send(0)

    def attend(m):
        factor = lax.rsqrt(total[:, width : width + hd] / D + 1e-05)
        heads = [total[:, h * hd : (h + 1) * hd] * factor for h in range(per_group + 2)]
        cos = cos8[m]
        sin = sin8[m]

        def rotate(x):
            return (x * cos + pltpu.roll(x, hd // 2, 1) * sin).astype(jnp.bfloat16)

        queries = rotate(jnp.concatenate(heads[:per_group], axis=0))
        new_key = rotate(jnp.concatenate([heads[per_group]] * per_group, axis=0))
        new_value = jnp.concatenate([heads[per_group + 1]] * per_group, axis=0)
        new_value = new_value.astype(jnp.bfloat16).astype(jnp.float32)
        which = lax.rem(row8, seqs)
        scores = None
        for b in range(seqs):
            mine = lax.dot_general(
                queries,
                keys[m, b],
                (((1,), (1,)), ((), ())),
                preferred_element_type=jnp.float32,
            )
            scores = mine if b == 0 else jnp.where(which == b, mine, scores)
        scores = scores * score_scale
        own = queries.astype(jnp.float32) * new_key.astype(jnp.float32)
        own = jnp.sum(own, axis=1, keepdims=True) * score_scale
        scores = jnp.where(lane < lengths_of(m), scores, -jnp.inf)
        top = jnp.maximum(jnp.max(scores, axis=1, keepdims=True), own)
        cache_exp = jnp.exp(scores - top)
        own_exp = jnp.exp(own - top)
        denom = jnp.sum(cache_exp, axis=1, keepdims=True) + own_exp
        weight = (cache_exp / denom).astype(jnp.bfloat16)
        own_weight = (own_exp / denom).astype(jnp.bfloat16).astype(jnp.float32)
        result = None
        for b in range(seqs):
            mine = jnp.dot(weight, vals[m, b], preferred_element_type=jnp.float32)
            result = mine if b == 0 else jnp.where(which == b, mine, result)
        return (result + own_weight * new_value).astype(jnp.bfloat16)

    def middle(m):
        @pl.when(in_feat)
        def _():
            pltpu.make_async_copy(rs_in.at[m], rs_in.at[m], rs_recv.at[m]).wait()
            whole = rs_out[m, c]
            for j in range(n_col - 1):
                whole = whole + rs_in[m, j]
            total[...] = whole

        @pl.when(in_seq)
        def _():
            value = take_state(m)
            squares, scaled = scale(value)
            across = jnp.concatenate(
                [scaled[k * seqs : (k + 1) * seqs] for k in range(n_blocks)], axis=1
            )
            total[:, 0:width] = jnp.dot(across, wq[...], preferred_element_type=jnp.float32)
            both = squares[0:seqs]
            for k in range(1, n_blocks):
                both = both + squares[k * seqs : (k + 1) * seqs]
            both = jnp.sum(both, axis=1, keepdims=True)
            total[:, width : width + hd] = jnp.broadcast_to(both, (seqs, hd))

        result = attend(m)

        @pl.when(out_feat)
        def _():
            for h in range(per_group):
                att[m, c, :, h * hd : (h + 1) * hd] = result[h * seqs : (h + 1) * seqs]
            for j in far_first(n_col):
                pltpu.make_async_remote_copy(
                    src_ref=att.at[m, c],
                    dst_ref=att.at[m, c],
                    send_sem=att_send.at[m],
                    recv_sem=att_recv.at[m],
                    device_id=at(s, r, lax.rem(c + j, n_col)),
                    device_id_type=MESH,
                ).start()

        @pl.when(out_seq)
        def _():
            flat = jnp.concatenate(
                [result[h * seqs : (h + 1) * seqs] for h in range(per_group)], axis=1
            )
            for k in range(n_blocks):
                mixed = jnp.dot(flat, wo[k], preferred_element_type=jnp.float32)
                po[m, k * seqs : (k + 1) * seqs] = mixed.astype(jnp.bfloat16)
            send_rows(m)

        @pl.when(in_seq)
        def _():
            pass_on(m)


    def mix_features(m):
        others = att.at[m, pl.ds(0, n_col - 1)]
        pltpu.make_async_copy(others, others, att_recv.at[m]).wait()
        mixed = jnp.dot(rows_of(att, m, n_col), wo[c], preferred_element_type=jnp.float32)
        mixed = mixed.astype(jnp.bfloat16)
        po[m] = mixed

        @pl.when(s == last)
        def _():
            pin[1, m, r] = mixed

        send_rows(m)

    def step(t, carry):
        @pl.when(in_feat & (t < micro))
        def _():
            project_features(t)

        @pl.when((t >= 2) & (t < micro + 2))
        def _():
            middle(t - 2)

        @pl.when(out_feat & (t >= 4))
        def _():
            mix_features(t - 4)

        return carry

    lax.fori_loop(0, micro + 4, step, 0)

    def finish(m, carry):
        @pl.when(s == last)
        def _():
            others = pin.at[1, m, pl.ds(0, n_row - 1)]
            pltpu.make_async_copy(others, others, po_recv.at[1, m]).wait()
            if last - 1 in BY_SEQUENCE:
                blocks = given.at[m, pl.ds(0, n_col - 1)]
                pltpu.make_async_copy(blocks, blocks, out_recv.at[m]).wait()
                pltpu.make_async_copy(blocks, blocks, prev_send.at[m]).wait()
                base = rows_of(given, m, n_blocks)
            else:
                base = rows[m]
            out_ref[m] = summed(1, m, base)
            pltpu.make_async_copy(others, others, po_send.at[m]).wait()

        @pl.when(s < last)
        def _():
            pltpu.make_async_copy(given.at[m], given.at[m], out_recv.at[m]).wait()
            out_ref[m] = rows_of(given, m, n_blocks)
            pltpu.make_async_copy(state.at[m], state.at[m], prev_send.at[m]).wait()
            pltpu.make_async_copy(pin.at[0, m], pin.at[0, m], po_send.at[m]).wait()

        @pl.when(s > 0)
        def _():
            pltpu.make_async_copy(state.at[m], state.at[m], out_send.at[m]).wait()

        @pl.when(in_feat)
        def _():
            pltpu.make_async_copy(rs_in.at[m], rs_in.at[m], rs_send.at[m]).wait()

        @pl.when(out_feat)
        def _():
            others = att.at[m, pl.ds(0, n_col - 1)]
            pltpu.make_async_copy(others, others, att_send.at[m]).wait()

        return carry

    lax.fori_loop(0, micro, finish, 0)


def solution(mesh):
    n_sec, n_row, n_col = mesh.shape["section"], mesh.shape["row"], mesh.shape["col"]

    def shards(hidden, norm_gain, w_qkv, w_out, cache_keys, cache_values, cache_lengths):
        micro, batch, feats = hidden.shape
        wq = w_qkv[0]
        wo = w_out[0]
        width = wq.shape[1]
        _, _, seqs, length, groups, hd = cache_keys.shape
        keys = cache_keys.reshape(micro, seqs, length, hd)
        vals = cache_values.reshape(micro, seqs, length, hd)
        rows8 = HEADS // KVH * seqs
        bf, f32 = jnp.bfloat16, jnp.float32
        vmem = pl.BlockSpec(memory_space=pltpu.VMEM)
        hbm = pl.BlockSpec(memory_space=pltpu.HBM)
        sem = pltpu.SemaphoreType.DMA
        out = pl.pallas_call(
            functools.partial(kernel, (n_sec, n_row, n_col)),
            out_shape=jax.ShapeDtypeStruct((micro, batch, feats), bf),
            in_specs=[hbm] * 7,
            out_specs=vmem,
            scratch_shapes=[
                pltpu.SMEM((seqs, micro), jnp.int32),
                pltpu.VMEM(hidden.shape, bf),
                pltpu.VMEM(norm_gain.shape, bf),
                pltpu.VMEM((n_col * feats, width), bf),
                pltpu.VMEM((n_col, *wo.shape), bf),
                pltpu.VMEM(keys.shape, bf),
                pltpu.VMEM(vals.shape, bf),
                pltpu.VMEM((micro, rows8, hd), f32),
                pltpu.VMEM((micro, rows8, hd), f32),
                pltpu.VMEM((n_col, 1, feats), bf),
                pltpu.VMEM((batch, feats), f32),
                pltpu.VMEM((micro, batch, feats), bf),
                pltpu.VMEM((micro, n_col, seqs, feats), bf),
                pltpu.VMEM((micro, n_col, seqs, feats), bf),
                pltpu.VMEM((micro, n_col, seqs, feats), bf),
                pltpu.VMEM((2, micro, n_row, batch, feats), bf),
                pltpu.VMEM((micro, n_col, seqs, width + hd), f32),
                pltpu.VMEM((micro, n_col - 1, seqs, width + hd), f32),
                pltpu.VMEM((seqs, width + hd), f32),
                pltpu.VMEM((micro, n_col, seqs, wo.shape[0]), bf),
                pltpu.VMEM((micro, batch, feats), bf),
                sem((7,)),
                sem,
                sem((2, n_col // 2, CHUNKS)),
                sem,
                sem((2, n_col // 2, CHUNKS)),
                sem,
                sem,
                pltpu.SemaphoreType.REGULAR,
                sem((micro,)),
                sem((micro,)),
                sem((micro,)),
                sem((micro,)),
                sem((micro,)),
                sem((2, micro)),
                sem((micro,)),
                sem((micro,)),
                sem((micro,)),
                sem((micro,)),
            ],
            compiler_params=pltpu.CompilerParams(
                collective_id=0, has_side_effects=True, vmem_limit_bytes=67000000
            ),
        )(cache_lengths.T, hidden, norm_gain, wq, wo, keys, vals)
        return out[None]

    return jax.shard_map(
        shards,
        mesh=mesh,
        in_specs=(
            P(None, None, "col"),
            P("section", "col"),
            P("section", "col", "row"),
            P("section", "row", "col"),
            P("section", None, "col", None, "row", None),
            P("section", None, "col", None, "row", None),
            P(None, "col"),
        ),
        out_specs=P("section", None, None, "col"),
        check_vma=False,
    )
```

```python
import functools
import math

import jax
import jax.numpy as jnp
from jax import lax
from jax.experimental import pallas as pl
from jax.experimental.pallas import tpu as pltpu
from jax.sharding import PartitionSpec as P

D = 4096
HEADS = 32
KVH = 8
MESH = pl.DeviceIdType.MESH
BY_SEQUENCE = (3, 5, 6)
CHUNKS = 4


def far_first(n):
    order = []
    for k in range(n // 2, 0, -1):
        order.append(k)
        if n - k != k:
            order.append(n - k)
    return order


def one_of(value, choices):
    hit = value < 0
    for choice in choices:
        hit = hit | (value == choice)
    return hit


def rows_of(ref, index, count):
    return jnp.concatenate([ref[index, k] for k in range(count)], axis=0)


def kernel(
    sizes,
    lens_hbm,
    hidden_hbm,
    gain_hbm,
    wq_hbm,
    wo_hbm,
    keys_hbm,
    vals_hbm,
    out_ref,
    lens_ref,
    hidden_ref,
    gain_ref,
    wq,
    wo,
    keys,
    vals,
    cos8,
    sin8,
    gains,
    gain32,
    rows,
    state,
    prev,
    given,
    pin,
    rs_out,
    rs_in,
    total,
    att,
    po,
    load_sem,
    wq_send,
    wq_recv,
    wo_send,
    wo_recv,
    gain_send,
    gain_recv,
    go_sem,
    rs_send,
    rs_recv,
    att_send,
    att_recv,
    po_send,
    po_recv,
    prev_send,
    prev_recv,
    out_send,
    out_recv,
):
    n_sec, n_row, n_col = sizes
    s = lax.axis_index("section")
    r = lax.axis_index("row")
    c = lax.axis_index("col")
    last = n_sec - 1
    micro, n_blocks, seqs, feats = state.shape
    batch = n_col * seqs
    hd = keys.shape[-1]
    width = wq.shape[1]
    per_group = HEADS // KVH
    rows8 = per_group * seqs
    out_seq = one_of(s, BY_SEQUENCE)
    out_feat = jnp.logical_not(out_seq)
    in_seq = one_of(s, [b + 1 for b in BY_SEQUENCE])
    in_feat = jnp.logical_not(in_seq)
    right, left = lax.rem(c + 1, n_col), lax.rem(c + n_col - 1, n_col)

    def at(sec, row, col):
        return {"section": sec, "row": row, "col": col}

    my_rows = pl.ds(pl.multiple_of(c * feats, feats), feats)
    load_wq = pltpu.make_async_copy(wq_hbm, wq.at[my_rows], load_sem.at[0])
    load_wo = pltpu.make_async_copy(wo_hbm, wo.at[c], load_sem.at[1])
    load_keys = pltpu.make_async_copy(keys_hbm, keys, load_sem.at[2])
    load_vals = pltpu.make_async_copy(vals_hbm, vals, load_sem.at[3])
    load_lens = pltpu.make_async_copy(lens_hbm, lens_ref, load_sem.at[4])
    load_gain = pltpu.make_async_copy(gain_hbm, gain_ref, load_sem.at[5])
    load_hidden = pltpu.make_async_copy(hidden_hbm, hidden_ref, load_sem.at[6])
    load_lens.start()
    load_gain.start()
    load_hidden.start()
    load_wq.start()
    load_wo.start()
    load_keys.start()
    load_vals.start()

    barrier = pltpu.get_barrier_semaphore()

    def greet(device):
        pl.semaphore_signal(barrier, inc=1, device_id=device, device_id_type=MESH)

    for j in far_first(n_col):
        greet(at(s, r, lax.rem(c + j, n_col)))

    @pl.when(s < last)
    def _():
        for j in range(n_row):
            greet(at(s + 1, lax.rem(r + j, n_row), c))
        for j in range(1, n_col):
            greet(at(s + 1, r, lax.rem(c + j, n_col)))

    @pl.when(s > 0)
    def _():
        for j in range(n_row):
            greet(at(s - 1, lax.rem(r + j, n_row), c))
        for j in range(1, n_col):
            greet(at(s - 1, r, lax.rem(c + j, n_col)))

    @pl.when(s == last)
    def _():
        for j in range(1, n_row):
            greet(at(s, lax.rem(r + j, n_row), c))

    load_lens.wait()
    load_gain.wait()
    load_hidden.wait()

    lane = lax.broadcasted_iota(jnp.int32, (rows8, hd), 1)
    row8 = lax.broadcasted_iota(jnp.int32, (rows8, hd), 0)
    half = lax.rem(lane, hd // 2).astype(jnp.float32)
    inverse_freq = jnp.exp(half * (-2.0 / hd * math.log(500000.0)))
    sign = jnp.where(lane < hd // 2, -1.0, 1.0)

    def lengths_of(m):
        value = jnp.full((rows8, hd), lens_ref[0, m], jnp.int32)
        for b in range(1, seqs):
            value = jnp.where(lax.rem(row8, seqs) == b, lens_ref[b, m], value)
        return value

    for m in range(micro):
        angle = lengths_of(m).astype(jnp.float32) * inverse_freq
        cos8[m] = jnp.cos(angle)
        sin8[m] = jnp.sin(angle) * sign
    gain32[...] = jnp.broadcast_to(gain_ref[...].astype(jnp.float32), gain32.shape)
    gains[c] = gain_ref[...]

    load_wq.wait()
    load_wo.wait()
    across = n_row + n_col - 1
    pl.semaphore_wait(
        barrier,
        n_col
        - 1
        + jnp.where(s < last, across, 0)
        + jnp.where(s > 0, across, 0)
        + jnp.where(s == last, n_row - 1, 0),
    )

    def gather(part, send_sem, recv_sem):
        def copy(way, step, block, piece, to):
            return pltpu.make_async_remote_copy(
                src_ref=part(block, piece),
                dst_ref=part(block, piece),
                send_sem=send_sem,
                recv_sem=recv_sem.at[way, step, piece],
                device_id=at(s, r, to),
                device_id_type=MESH,
            )

        def arrived(way, step, piece):
            pltpu.make_async_copy(part(0, 0), part(0, 0), recv_sem.at[way, step, piece]).wait()

        for piece in range(CHUNKS):
            copy(0, 0, c, piece, right).start()
            copy(1, 0, c, piece, left).start()

        steps = n_col // 2

        def forward(step, carry):
            for piece in range(CHUNKS):
                arrived(0, step - 1, piece)

                @pl.when((step < steps - 1) | (piece < CHUNKS // 2))
                def _():
                    copy(0, step, lax.rem(c + n_col - step, n_col), piece, right).start()

                arrived(1, step - 1, piece)

                @pl.when((step < steps - 1) | (piece >= CHUNKS // 2))
                def _():
                    copy(1, step, lax.rem(c + step, n_col), piece, left).start()

            return carry

        lax.fori_loop(1, steps, forward, 0)
        for piece in range(CHUNKS):
            arrived(0 if piece < CHUNKS // 2 else 1, steps - 1, piece)

        def sent(k, carry):
            for piece in range(CHUNKS):
                pltpu.make_async_copy(part(0, 0), part(0, 0), send_sem).wait()
            return carry

        lax.fori_loop(0, n_col - 1, sent, 0)

    piece_rows = feats // CHUNKS

    def wq_part(block, piece):
        first = pl.multiple_of(block * feats + piece * piece_rows, piece_rows)
        return wq.at[pl.ds(first, piece_rows)]

    wo_rows = wo.shape[1] // CHUNKS

    def wo_part(block, piece):
        return wo.at[block, pl.ds(piece * wo_rows, wo_rows)]

    odd = lax.rem(s, 2) == 1

    @pl.when(odd & (s > 1))
    def _():
        pl.semaphore_wait(go_sem, 1)

    @pl.when(in_seq)
    def _():
        for j in far_first(n_col):
            pltpu.make_async_remote_copy(
                src_ref=gains.at[c],
                dst_ref=gains.at[c],
                send_sem=gain_send,
                recv_sem=gain_recv,
                device_id=at(s, r, lax.rem(c + j, n_col)),
                device_id_type=MESH,
            ).start()
        gather(wq_part, wq_send, wq_recv)
        others = gains.at[pl.ds(0, n_col - 1)]
        pltpu.make_async_copy(others, others, gain_recv).wait()
        pltpu.make_async_copy(others, others, gain_send).wait()
        for k in range(n_col):
            gain32[k * seqs : (k + 1) * seqs] = jnp.broadcast_to(
                gains[k].astype(jnp.float32), (seqs, feats)
            )

    @pl.when(out_seq)
    def _():
        gather(wo_part, wo_send, wo_recv)

    @pl.when(jnp.logical_not(odd) & (s > 0))
    def _():
        pl.semaphore_signal(go_sem, inc=1, device_id=at(s + 1, r, c), device_id_type=MESH)

    load_keys.wait()
    load_vals.wait()
    score_scale = 1.0 / math.sqrt(hd)

    def summed(region, m, base):
        mixed = pin[region, m, 0]
        for k in range(1, n_row):
            mixed = mixed + pin[region, m, k]
        return (base.astype(jnp.float32) + mixed).astype(jnp.bfloat16)

    def hand_over(m, to_section, buffer, same, send_sem, recv_sem):
        @pl.when(same)
        def _():
            pltpu.make_async_remote_copy(
                src_ref=state.at[m],
                dst_ref=buffer.at[m],
                send_sem=send_sem.at[m],
                recv_sem=recv_sem.at[m],
                device_id=at(to_section, r, c),
                device_id_type=MESH,
            ).start()

        @pl.when(jnp.logical_not(same))
        def _():
            for j in [*far_first(n_col), 0]:
                to = lax.rem(c + j, n_col)
                pltpu.make_async_remote_copy(
                    src_ref=state.at[m, to],
                    dst_ref=buffer.at[m, c],
                    send_sem=send_sem.at[m],
                    recv_sem=recv_sem.at[m],
                    device_id=at(to_section, r, to),
                    device_id_type=MESH,
                ).start()

    def take_state(m):
        @pl.when(s == 0)
        def _():
            rows[m] = hidden_ref[m]

        @pl.when(s > 0)
        def _():
            pltpu.make_async_copy(prev.at[m], prev.at[m], prev_recv.at[m]).wait()
            base = rows_of(prev, m, n_blocks)
            pltpu.make_async_copy(pin.at[0, m], pin.at[0, m], po_recv.at[0, m]).wait()
            rows[m] = summed(0, m, base)

        return rows[m]

    def pass_on(m):
        value = rows[m]
        for k in range(n_blocks):
            state[m, k] = value[k * seqs : (k + 1) * seqs]

        @pl.when(s < last)
        def _():
            hand_over(m, s + 1, prev, in_seq == out_seq, prev_send, prev_recv)

        @pl.when(s > 0)
        def _():
            hand_over(m, s - 1, given, in_feat, out_send, out_recv)

        @pl.when((s == last) & in_seq)
        def _():
            given[m, c] = state[m, c]
            for j in far_first(n_col):
                to = lax.rem(c + j, n_col)
                pltpu.make_async_remote_copy(
                    src_ref=state.at[m, to],
                    dst_ref=given.at[m, c],
                    send_sem=prev_send.at[m],
                    recv_sem=out_recv.at[m],
                    device_id=at(s, r, to),
                    device_id_type=MESH,
                ).start()

    def scale(value):
        h_float = value.astype(jnp.float32)
        return h_float * h_float, (h_float * gain32[...]).astype(jnp.bfloat16)

    def project_features(m):
        value = take_state(m)
        squares, scaled = scale(value)
        own_rows = pl.ds(pl.multiple_of(c * feats, feats), feats)
        partial = jnp.dot(scaled, wq[own_rows, :], preferred_element_type=jnp.float32)
        squares = jnp.sum(squares, axis=1, keepdims=True)
        squares = jnp.broadcast_to(squares, (batch, hd))
        for k in range(n_col):
            rs_out[m, k, :, 0:width] = partial[k * seqs : (k + 1) * seqs]
            rs_out[m, k, :, width : width + hd] = squares[k * seqs : (k + 1) * seqs]
        for j in far_first(n_col):
            to = lax.rem(c + j, n_col)
            pltpu.make_async_remote_copy(
                src_ref=rs_out.at[m, to],
                dst_ref=rs_in.at[m, j - 1],
                send_sem=rs_send.at[m],
                recv_sem=rs_recv.at[m],
                device_id=at(s, r, to),
                device_id_type=MESH,
            ).start()
        pass_on(m)

    region = jnp.where(s == last, 1, 0)
    target = jnp.where(s == last, last, s + 1)

    def send_rows(m):
        def send(j):
            pltpu.make_async_remote_copy(
                src_ref=po.at[m],
                dst_ref=pin.at[region, m, r],
                send_sem=po_send.at[m],
                recv_sem=po_recv.at[region, m],
                device_id=at(target, lax.rem(r + j, n_row), c),
                device_id_type=MESH,
            ).start()

        for j in far_first(n_row):
            send(j)

        @pl.when(s < last)
        def _():
            send(0)

    def attend(m):
        factor = lax.rsqrt(total[:, width : width + hd] / D + 1e-05)
        heads = [total[:, h * hd : (h + 1) * hd] * factor for h in range(per_group + 2)]
        cos = cos8[m]
        sin = sin8[m]

        def rotate(x):
            return (x * cos + pltpu.roll(x, hd // 2, 1) * sin).astype(jnp.bfloat16)

        queries = rotate(jnp.concatenate(heads[:per_group], axis=0))
        new_key = rotate(jnp.concatenate([heads[per_group]] * per_group, axis=0))
        new_value = jnp.concatenate([heads[per_group + 1]] * per_group, axis=0)
        new_value = new_value.astype(jnp.bfloat16).astype(jnp.float32)
        which = lax.rem(row8, seqs)
        scores = None
        for b in range(seqs):
            mine = lax.dot_general(
                queries,
                keys[m, b],
                (((1,), (1,)), ((), ())),
                preferred_element_type=jnp.float32,
            )
            scores = mine if b == 0 else jnp.where(which == b, mine, scores)
        scores = scores * score_scale
        own = queries.astype(jnp.float32) * new_key.astype(jnp.float32)
        own = jnp.sum(own, axis=1, keepdims=True) * score_scale
        scores = jnp.where(lane < lengths_of(m), scores, -jnp.inf)
        top = jnp.maximum(jnp.max(scores, axis=1, keepdims=True), own)
        cache_exp = jnp.exp(scores - top)
        own_exp = jnp.exp(own - top)
        denom = jnp.sum(cache_exp, axis=1, keepdims=True) + own_exp
        weight = (cache_exp / denom).astype(jnp.bfloat16)
        own_weight = (own_exp / denom).astype(jnp.bfloat16).astype(jnp.float32)
        result = None
        for b in range(seqs):
            mine = jnp.dot(weight, vals[m, b], preferred_element_type=jnp.float32)
            result = mine if b == 0 else jnp.where(which == b, mine, result)
        return (result + own_weight * new_value).astype(jnp.bfloat16)

    def middle(m):
        @pl.when(in_feat)
        def _():
            pltpu.make_async_copy(rs_in.at[m], rs_in.at[m], rs_recv.at[m]).wait()
            whole = rs_out[m, c]
            for j in range(n_col - 1):
                whole = whole + rs_in[m, j]
            total[...] = whole

        @pl.when(in_seq)
        def _():
            value = take_state(m)
            squares, scaled = scale(value)
            across = jnp.concatenate(
                [scaled[k * seqs : (k + 1) * seqs] for k in range(n_blocks)], axis=1
            )
            total[:, 0:width] = jnp.dot(across, wq[...], preferred_element_type=jnp.float32)
            both = squares[0:seqs]
            for k in range(1, n_blocks):
                both = both + squares[k * seqs : (k + 1) * seqs]
            both = jnp.sum(both, axis=1, keepdims=True)
            total[:, width : width + hd] = jnp.broadcast_to(both, (seqs, hd))

        result = attend(m)

        @pl.when(out_feat)
        def _():
            for h in range(per_group):
                att[m, c, :, h * hd : (h + 1) * hd] = result[h * seqs : (h + 1) * seqs]
            for j in far_first(n_col):
                pltpu.make_async_remote_copy(
                    src_ref=att.at[m, c],
                    dst_ref=att.at[m, c],
                    send_sem=att_send.at[m],
                    recv_sem=att_recv.at[m],
                    device_id=at(s, r, lax.rem(c + j, n_col)),
                    device_id_type=MESH,
                ).start()

        @pl.when(out_seq)
        def _():
            flat = jnp.concatenate(
                [result[h * seqs : (h + 1) * seqs] for h in range(per_group)], axis=1
            )
            for k in range(n_blocks):
                mixed = jnp.dot(flat, wo[k], preferred_element_type=jnp.float32)
                po[m, k * seqs : (k + 1) * seqs] = mixed
            send_rows(m)

        @pl.when(in_seq)
        def _():
            pass_on(m)


    def mix_features(m):
        others = att.at[m, pl.ds(0, n_col - 1)]
        pltpu.make_async_copy(others, others, att_recv.at[m]).wait()
        mixed = jnp.dot(rows_of(att, m, n_col), wo[c], preferred_element_type=jnp.float32)
        po[m] = mixed

        @pl.when(s == last)
        def _():
            pin[1, m, r] = mixed

        send_rows(m)

    def step(t, carry):
        @pl.when(in_feat & (t < micro))
        def _():
            project_features(t)

        @pl.when((t >= 2) & (t < micro + 2))
        def _():
            middle(t - 2)

        @pl.when(out_feat & (t >= 4))
        def _():
            mix_features(t - 4)

        return carry

    lax.fori_loop(0, micro + 4, step, 0)

    def finish(m, carry):
        @pl.when(s == last)
        def _():
            others = pin.at[1, m, pl.ds(0, n_row - 1)]
            pltpu.make_async_copy(others, others, po_recv.at[1, m]).wait()
            if last - 1 in BY_SEQUENCE:
                blocks = given.at[m, pl.ds(0, n_col - 1)]
                pltpu.make_async_copy(blocks, blocks, out_recv.at[m]).wait()
                pltpu.make_async_copy(blocks, blocks, prev_send.at[m]).wait()
                base = rows_of(given, m, n_blocks)
            else:
                base = rows[m]
            out_ref[m] = summed(1, m, base)
            pltpu.make_async_copy(others, others, po_send.at[m]).wait()

        @pl.when(s < last)
        def _():
            pltpu.make_async_copy(given.at[m], given.at[m], out_recv.at[m]).wait()
            out_ref[m] = rows_of(given, m, n_blocks)
            pltpu.make_async_copy(state.at[m], state.at[m], prev_send.at[m]).wait()
            pltpu.make_async_copy(pin.at[0, m], pin.at[0, m], po_send.at[m]).wait()

        @pl.when(s > 0)
        def _():
            pltpu.make_async_copy(state.at[m], state.at[m], out_send.at[m]).wait()

        @pl.when(in_feat)
        def _():
            pltpu.make_async_copy(rs_in.at[m], rs_in.at[m], rs_send.at[m]).wait()

        @pl.when(out_feat)
        def _():
            others = att.at[m, pl.ds(0, n_col - 1)]
            pltpu.make_async_copy(others, others, att_send.at[m]).wait()

        return carry

    lax.fori_loop(0, micro, finish, 0)


def solution(mesh):
    n_sec, n_row, n_col = mesh.shape["section"], mesh.shape["row"], mesh.shape["col"]

    def shards(hidden, norm_gain, w_qkv, w_out, cache_keys, cache_values, cache_lengths):
        micro, batch, feats = hidden.shape
        wq = w_qkv[0]
        wo = w_out[0]
        width = wq.shape[1]
        _, _, seqs, length, groups, hd = cache_keys.shape
        keys = cache_keys.reshape(micro, seqs, length, hd)
        vals = cache_values.reshape(micro, seqs, length, hd)
        rows8 = HEADS // KVH * seqs
        bf, f32 = jnp.bfloat16, jnp.float32
        vmem = pl.BlockSpec(memory_space=pltpu.VMEM)
        hbm = pl.BlockSpec(memory_space=pltpu.HBM)
        sem = pltpu.SemaphoreType.DMA
        out = pl.pallas_call(
            functools.partial(kernel, (n_sec, n_row, n_col)),
            out_shape=jax.ShapeDtypeStruct((micro, batch, feats), bf),
            in_specs=[hbm] * 7,
            out_specs=vmem,
            scratch_shapes=[
                pltpu.SMEM((seqs, micro), jnp.int32),
                pltpu.VMEM(hidden.shape, bf),
                pltpu.VMEM(norm_gain.shape, bf),
                pltpu.VMEM((n_col * feats, width), bf),
                pltpu.VMEM((n_col, *wo.shape), bf),
                pltpu.VMEM(keys.shape, bf),
                pltpu.VMEM(vals.shape, bf),
                pltpu.VMEM((micro, rows8, hd), f32),
                pltpu.VMEM((micro, rows8, hd), f32),
                pltpu.VMEM((n_col, 1, feats), bf),
                pltpu.VMEM((batch, feats), f32),
                pltpu.VMEM((micro, batch, feats), bf),
                pltpu.VMEM((micro, n_col, seqs, feats), bf),
                pltpu.VMEM((micro, n_col, seqs, feats), bf),
                pltpu.VMEM((micro, n_col, seqs, feats), bf),
                pltpu.VMEM((2, micro, n_row, batch, feats), f32),
                pltpu.VMEM((micro, n_col, seqs, width + hd), f32),
                pltpu.VMEM((micro, n_col - 1, seqs, width + hd), f32),
                pltpu.VMEM((seqs, width + hd), f32),
                pltpu.VMEM((micro, n_col, seqs, wo.shape[0]), bf),
                pltpu.VMEM((micro, batch, feats), f32),
                sem((7,)),
                sem,
                sem((2, n_col // 2, CHUNKS)),
                sem,
                sem((2, n_col // 2, CHUNKS)),
                sem,
                sem,
                pltpu.SemaphoreType.REGULAR,
                sem((micro,)),
                sem((micro,)),
                sem((micro,)),
                sem((micro,)),
                sem((micro,)),
                sem((2, micro)),
                sem((micro,)),
                sem((micro,)),
                sem((micro,)),
                sem((micro,)),
            ],
            compiler_params=pltpu.CompilerParams(
                collective_id=0, has_side_effects=True, vmem_limit_bytes=67000000
            ),
        )(cache_lengths.T, hidden, norm_gain, wq, wo, keys, vals)
        return out[None]

    return jax.shard_map(
        shards,
        mesh=mesh,
        in_specs=(
            P(None, None, "col"),
            P("section", "col"),
            P("section", "col", "row"),
            P("section", "row", "col"),
            P("section", None, "col", None, "row", None),
            P("section", None, "col", None, "row", None),
            P(None, "col"),
        ),
        out_specs=P("section", None, None, "col"),
        check_vma=False,
    )
```

```python
import functools
import math

import jax
import jax.numpy as jnp
from jax import lax
from jax.experimental import pallas as pl
from jax.experimental.pallas import tpu as pltpu
from jax.sharding import PartitionSpec as P

D = 4096
HEADS = 32
KVH = 8
MESH = pl.DeviceIdType.MESH
BY_SEQUENCE = (3, 5, 6)
CHUNKS = 4


def far_first(n):
    order = []
    for k in range(n // 2, 0, -1):
        order.append(k)
        if n - k != k:
            order.append(n - k)
    return order


def one_of(value, choices):
    hit = value < 0
    for choice in choices:
        hit = hit | (value == choice)
    return hit


def rows_of(ref, index, count):
    return jnp.concatenate([ref[index, k] for k in range(count)], axis=0)


def kernel(
    sizes,
    lens_hbm,
    hidden_hbm,
    gain_hbm,
    wq_hbm,
    wo_hbm,
    keys_hbm,
    vals_hbm,
    out_ref,
    lens_ref,
    hidden_ref,
    gain_ref,
    wq,
    wo,
    keys,
    vals,
    cos8,
    sin8,
    gains,
    gain32,
    rows,
    state,
    prev,
    given,
    pin,
    rs_out,
    rs_in,
    total,
    att,
    po,
    load_sem,
    wq_send,
    wq_recv,
    wo_send,
    wo_recv,
    gain_send,
    gain_recv,
    go_sem,
    rs_send,
    rs_recv,
    att_send,
    att_recv,
    po_send,
    po_recv,
    prev_send,
    prev_recv,
    out_send,
    out_recv,
):
    n_sec, n_row, n_col = sizes
    s = lax.axis_index("section")
    r = lax.axis_index("row")
    c = lax.axis_index("col")
    last = n_sec - 1
    micro, n_blocks, seqs, feats = state.shape
    batch = n_col * seqs
    hd = keys.shape[-1]
    width = wq.shape[1]
    per_group = HEADS // KVH
    rows8 = per_group * seqs
    out_seq = one_of(s, BY_SEQUENCE)
    out_feat = jnp.logical_not(out_seq)
    in_seq = one_of(s, [b + 1 for b in BY_SEQUENCE])
    in_feat = jnp.logical_not(in_seq)
    spread_out = in_seq | out_seq
    spread_in = in_seq | one_of(s, [b + 2 for b in BY_SEQUENCE])
    right, left = lax.rem(c + 1, n_col), lax.rem(c + n_col - 1, n_col)

    def at(sec, row, col):
        return {"section": sec, "row": row, "col": col}

    my_rows = pl.ds(pl.multiple_of(c * feats, feats), feats)
    load_wq = pltpu.make_async_copy(wq_hbm, wq.at[my_rows], load_sem.at[0])
    load_wo = pltpu.make_async_copy(wo_hbm, wo.at[c], load_sem.at[1])
    load_keys = pltpu.make_async_copy(keys_hbm, keys, load_sem.at[2])
    load_vals = pltpu.make_async_copy(vals_hbm, vals, load_sem.at[3])
    load_lens = pltpu.make_async_copy(lens_hbm, lens_ref, load_sem.at[4])
    load_gain = pltpu.make_async_copy(gain_hbm, gain_ref, load_sem.at[5])
    load_hidden = pltpu.make_async_copy(hidden_hbm, hidden_ref, load_sem.at[6])
    load_lens.start()
    load_gain.start()
    load_hidden.start()
    load_wq.start()
    load_wo.start()
    load_keys.start()
    load_vals.start()

    barrier = pltpu.get_barrier_semaphore()

    def greet(device):
        pl.semaphore_signal(barrier, inc=1, device_id=device, device_id_type=MESH)

    for j in far_first(n_col):
        greet(at(s, r, lax.rem(c + j, n_col)))

    @pl.when(s < last)
    def _():
        for j in range(n_row):
            greet(at(s + 1, lax.rem(r + j, n_row), c))

    @pl.when((s < last) & spread_out)
    def _():
        for j in range(1, n_col):
            greet(at(s + 1, r, lax.rem(c + j, n_col)))

    @pl.when(s > 0)
    def _():
        for j in range(n_row):
            greet(at(s - 1, lax.rem(r + j, n_row), c))

    @pl.when((s > 0) & spread_in)
    def _():
        for j in range(1, n_col):
            greet(at(s - 1, r, lax.rem(c + j, n_col)))

    @pl.when(s == last)
    def _():
        for j in range(1, n_row):
            greet(at(s, lax.rem(r + j, n_row), c))

    load_lens.wait()
    load_gain.wait()
    load_hidden.wait()

    lane = lax.broadcasted_iota(jnp.int32, (rows8, hd), 1)
    row8 = lax.broadcasted_iota(jnp.int32, (rows8, hd), 0)
    half = lax.rem(lane, hd // 2).astype(jnp.float32)
    inverse_freq = jnp.exp(half * (-2.0 / hd * math.log(500000.0)))
    sign = jnp.where(lane < hd // 2, -1.0, 1.0)

    def lengths_of(m):
        value = jnp.full((rows8, hd), lens_ref[0, m], jnp.int32)
        for b in range(1, seqs):
            value = jnp.where(lax.rem(row8, seqs) == b, lens_ref[b, m], value)
        return value

    for m in range(micro):
        angle = lengths_of(m).astype(jnp.float32) * inverse_freq
        cos8[m] = jnp.cos(angle)
        sin8[m] = jnp.sin(angle) * sign
    gain32[...] = jnp.broadcast_to(gain_ref[...].astype(jnp.float32), gain32.shape)
    gains[c] = gain_ref[...]

    load_wq.wait()
    load_wo.wait()
    pl.semaphore_wait(
        barrier,
        n_col
        - 1
        + jnp.where(s < last, n_row, 0)
        + jnp.where((s < last) & spread_out, n_col - 1, 0)
        + jnp.where(s > 0, n_row, 0)
        + jnp.where((s > 0) & spread_in, n_col - 1, 0)
        + jnp.where(s == last, n_row - 1, 0),
    )

    def gather(part, send_sem, recv_sem):
        def copy(way, step, block, piece, to):
            return pltpu.make_async_remote_copy(
                src_ref=part(block, piece),
                dst_ref=part(block, piece),
                send_sem=send_sem,
                recv_sem=recv_sem.at[way, step, piece],
                device_id=at(s, r, to),
                device_id_type=MESH,
            )

        def arrived(way, step, piece):
            pltpu.make_async_copy(part(0, 0), part(0, 0), recv_sem.at[way, step, piece]).wait()

        for piece in range(CHUNKS):
            copy(0, 0, c, piece, right).start()
            copy(1, 0, c, piece, left).start()

        steps = n_col // 2

        def forward(step, carry):
            for piece in range(CHUNKS):
                arrived(0, step - 1, piece)

                @pl.when((step < steps - 1) | (piece < CHUNKS // 2))
                def _():
                    copy(0, step, lax.rem(c + n_col - step, n_col), piece, right).start()

                arrived(1, step - 1, piece)

                @pl.when((step < steps - 1) | (piece >= CHUNKS // 2))
                def _():
                    copy(1, step, lax.rem(c + step, n_col), piece, left).start()

            return carry

        lax.fori_loop(1, steps, forward, 0)
        for piece in range(CHUNKS):
            arrived(0 if piece < CHUNKS // 2 else 1, steps - 1, piece)

        def sent(k, carry):
            for piece in range(CHUNKS):
                pltpu.make_async_copy(part(0, 0), part(0, 0), send_sem).wait()
            return carry

        lax.fori_loop(0, n_col - 1, sent, 0)

    piece_rows = feats // CHUNKS

    def wq_part(block, piece):
        first = pl.multiple_of(block * feats + piece * piece_rows, piece_rows)
        return wq.at[pl.ds(first, piece_rows)]

    wo_rows = wo.shape[1] // CHUNKS

    def wo_part(block, piece):
        return wo.at[block, pl.ds(piece * wo_rows, wo_rows)]

    odd = lax.rem(s, 2) == 1

    @pl.when(odd & (s > 1))
    def _():
        pl.semaphore_wait(go_sem, 1)

    @pl.when(in_seq)
    def _():
        for j in far_first(n_col):
            pltpu.make_async_remote_copy(
                src_ref=gains.at[c],
                dst_ref=gains.at[c],
                send_sem=gain_send,
                recv_sem=gain_recv,
                device_id=at(s, r, lax.rem(c + j, n_col)),
                device_id_type=MESH,
            ).start()
        gather(wq_part, wq_send, wq_recv)
        others = gains.at[pl.ds(0, n_col - 1)]
        pltpu.make_async_copy(others, others, gain_recv).wait()
        pltpu.make_async_copy(others, others, gain_send).wait()
        for k in range(n_col):
            gain32[k * seqs : (k + 1) * seqs] = jnp.broadcast_to(
                gains[k].astype(jnp.float32), (seqs, feats)
            )

    @pl.when(out_seq)
    def _():
        gather(wo_part, wo_send, wo_recv)

    @pl.when(jnp.logical_not(odd) & (s > 0))
    def _():
        pl.semaphore_signal(go_sem, inc=1, device_id=at(s + 1, r, c), device_id_type=MESH)

    load_keys.wait()
    load_vals.wait()
    score_scale = 1.0 / math.sqrt(hd)

    def summed(region, m, base):
        mixed = pin[region, m, 0].astype(jnp.float32)
        for k in range(1, n_row):
            mixed = mixed + pin[region, m, k].astype(jnp.float32)
        return (base.astype(jnp.float32) + mixed).astype(jnp.bfloat16)

    def hand_over(m, to_section, buffer, same, send_sem, recv_sem):
        @pl.when(same)
        def _():
            pltpu.make_async_remote_copy(
                src_ref=state.at[m],
                dst_ref=buffer.at[m],
                send_sem=send_sem.at[m],
                recv_sem=recv_sem.at[m],
                device_id=at(to_section, r, c),
                device_id_type=MESH,
            ).start()

        @pl.when(jnp.logical_not(same))
        def _():
            for j in [*far_first(n_col), 0]:
                to = lax.rem(c + j, n_col)
                pltpu.make_async_remote_copy(
                    src_ref=state.at[m, to],
                    dst_ref=buffer.at[m, c],
                    send_sem=send_sem.at[m],
                    recv_sem=recv_sem.at[m],
                    device_id=at(to_section, r, to),
                    device_id_type=MESH,
                ).start()

    def take_state(m):
        @pl.when(s == 0)
        def _():
            rows[m] = hidden_ref[m]

        @pl.when(s > 0)
        def _():
            pltpu.make_async_copy(prev.at[m], prev.at[m], prev_recv.at[m]).wait()
            base = rows_of(prev, m, n_blocks)
            pltpu.make_async_copy(pin.at[0, m], pin.at[0, m], po_recv.at[0, m]).wait()
            rows[m] = summed(0, m, base)

        return rows[m]

    def pass_on(m):
        value = rows[m]
        for k in range(n_blocks):
            state[m, k] = value[k * seqs : (k + 1) * seqs]

        @pl.when(s < last)
        def _():
            hand_over(m, s + 1, prev, in_seq == out_seq, prev_send, prev_recv)

        @pl.when(s > 0)
        def _():
            hand_over(m, s - 1, given, in_feat, out_send, out_recv)

        @pl.when((s == last) & in_seq)
        def _():
            given[m, c] = state[m, c]
            for j in far_first(n_col):
                to = lax.rem(c + j, n_col)
                pltpu.make_async_remote_copy(
                    src_ref=state.at[m, to],
                    dst_ref=given.at[m, c],
                    send_sem=prev_send.at[m],
                    recv_sem=out_recv.at[m],
                    device_id=at(s, r, to),
                    device_id_type=MESH,
                ).start()

    def scale(value):
        h_float = value.astype(jnp.float32)
        return h_float * h_float, (h_float * gain32[...]).astype(jnp.bfloat16)

    def project_features(m):
        value = take_state(m)
        squares, scaled = scale(value)
        own_rows = pl.ds(pl.multiple_of(c * feats, feats), feats)
        partial = jnp.dot(scaled, wq[own_rows, :], preferred_element_type=jnp.float32)
        squares = jnp.sum(squares, axis=1, keepdims=True)
        squares = jnp.broadcast_to(squares, (batch, hd))
        for k in range(n_col):
            rs_out[m, k, :, 0:width] = partial[k * seqs : (k + 1) * seqs]
            rs_out[m, k, :, width : width + hd] = squares[k * seqs : (k + 1) * seqs]
        for j in far_first(n_col):
            to = lax.rem(c + j, n_col)
            pltpu.make_async_remote_copy(
                src_ref=rs_out.at[m, to],
                dst_ref=rs_in.at[m, j - 1],
                send_sem=rs_send.at[m],
                recv_sem=rs_recv.at[m],
                device_id=at(s, r, to),
                device_id_type=MESH,
            ).start()
        pass_on(m)

    region = jnp.where(s == last, 1, 0)
    target = jnp.where(s == last, last, s + 1)

    def send_rows(m):
        def send(j):
            pltpu.make_async_remote_copy(
                src_ref=po.at[m],
                dst_ref=pin.at[region, m, r],
                send_sem=po_send.at[m],
                recv_sem=po_recv.at[region, m],
                device_id=at(target, lax.rem(r + j, n_row), c),
                device_id_type=MESH,
            ).start()

        for j in far_first(n_row):
            send(j)

        @pl.when(s < last)
        def _():
            send(0)

    def attend(m):
        factor = lax.rsqrt(total[:, width : width + hd] / D + 1e-05)
        heads = [total[:, h * hd : (h + 1) * hd] * factor for h in range(per_group + 2)]
        cos = cos8[m]
        sin = sin8[m]

        def rotate(x):
            return (x * cos + pltpu.roll(x, hd // 2, 1) * sin).astype(jnp.bfloat16)

        queries = rotate(jnp.concatenate(heads[:per_group], axis=0))
        new_key = rotate(jnp.concatenate([heads[per_group]] * per_group, axis=0))
        new_value = jnp.concatenate([heads[per_group + 1]] * per_group, axis=0)
        new_value = new_value.astype(jnp.bfloat16).astype(jnp.float32)
        which = lax.rem(row8, seqs)
        scores = None
        for b in range(seqs):
            mine = lax.dot_general(
                queries,
                keys[m, b],
                (((1,), (1,)), ((), ())),
                preferred_element_type=jnp.float32,
            )
            scores = mine if b == 0 else jnp.where(which == b, mine, scores)
        scores = scores * score_scale
        own = queries.astype(jnp.float32) * new_key.astype(jnp.float32)
        own = jnp.sum(own, axis=1, keepdims=True) * score_scale
        scores = jnp.where(lane < lengths_of(m), scores, -jnp.inf)
        top = jnp.maximum(jnp.max(scores, axis=1, keepdims=True), own)
        cache_exp = jnp.exp(scores - top)
        own_exp = jnp.exp(own - top)
        denom = jnp.sum(cache_exp, axis=1, keepdims=True) + own_exp
        weight = (cache_exp / denom).astype(jnp.bfloat16)
        own_weight = (own_exp / denom).astype(jnp.bfloat16).astype(jnp.float32)
        result = None
        for b in range(seqs):
            mine = jnp.dot(weight, vals[m, b], preferred_element_type=jnp.float32)
            result = mine if b == 0 else jnp.where(which == b, mine, result)
        return (result + own_weight * new_value).astype(jnp.bfloat16)

    def middle(m):
        @pl.when(in_feat)
        def _():
            pltpu.make_async_copy(rs_in.at[m], rs_in.at[m], rs_recv.at[m]).wait()
            whole = rs_out[m, c]
            for j in range(n_col - 1):
                whole = whole + rs_in[m, j]
            total[...] = whole

        @pl.when(in_seq)
        def _():
            value = take_state(m)
            squares, scaled = scale(value)
            across = jnp.concatenate(
                [scaled[k * seqs : (k + 1) * seqs] for k in range(n_blocks)], axis=1
            )
            total[:, 0:width] = jnp.dot(across, wq[...], preferred_element_type=jnp.float32)
            both = squares[0:seqs]
            for k in range(1, n_blocks):
                both = both + squares[k * seqs : (k + 1) * seqs]
            both = jnp.sum(both, axis=1, keepdims=True)
            total[:, width : width + hd] = jnp.broadcast_to(both, (seqs, hd))

        result = attend(m)

        @pl.when(out_feat)
        def _():
            for h in range(per_group):
                att[m, c, :, h * hd : (h + 1) * hd] = result[h * seqs : (h + 1) * seqs]
            for j in far_first(n_col):
                pltpu.make_async_remote_copy(
                    src_ref=att.at[m, c],
                    dst_ref=att.at[m, c],
                    send_sem=att_send.at[m],
                    recv_sem=att_recv.at[m],
                    device_id=at(s, r, lax.rem(c + j, n_col)),
                    device_id_type=MESH,
                ).start()

        @pl.when(out_seq)
        def _():
            flat = jnp.concatenate(
                [result[h * seqs : (h + 1) * seqs] for h in range(per_group)], axis=1
            )
            for k in range(n_blocks):
                mixed = jnp.dot(flat, wo[k], preferred_element_type=jnp.float32)
                po[m, k * seqs : (k + 1) * seqs] = mixed.astype(jnp.bfloat16)
            send_rows(m)

        @pl.when(in_seq)
        def _():
            pass_on(m)


    def mix_features(m):
        others = att.at[m, pl.ds(0, n_col - 1)]
        pltpu.make_async_copy(others, others, att_recv.at[m]).wait()
        mixed = jnp.dot(rows_of(att, m, n_col), wo[c], preferred_element_type=jnp.float32)
        mixed = mixed.astype(jnp.bfloat16)
        po[m] = mixed

        @pl.when(s == last)
        def _():
            pin[1, m, r] = mixed

        send_rows(m)

    def step(t, carry):
        @pl.when(in_feat & (t < micro))
        def _():
            project_features(t)

        @pl.when((t >= 2) & (t < micro + 2))
        def _():
            middle(t - 2)

        @pl.when(out_feat & (t >= 4))
        def _():
            mix_features(t - 4)

        return carry

    lax.fori_loop(0, micro + 4, step, 0)

    def finish(m, carry):
        @pl.when(s == last)
        def _():
            others = pin.at[1, m, pl.ds(0, n_row - 1)]
            pltpu.make_async_copy(others, others, po_recv.at[1, m]).wait()
            if last - 1 in BY_SEQUENCE:
                blocks = given.at[m, pl.ds(0, n_col - 1)]
                pltpu.make_async_copy(blocks, blocks, out_recv.at[m]).wait()
                pltpu.make_async_copy(blocks, blocks, prev_send.at[m]).wait()
                base = rows_of(given, m, n_blocks)
            else:
                base = rows[m]
            out_ref[m] = summed(1, m, base)
            pltpu.make_async_copy(others, others, po_send.at[m]).wait()

        @pl.when(s < last)
        def _():
            pltpu.make_async_copy(given.at[m], given.at[m], out_recv.at[m]).wait()
            out_ref[m] = rows_of(given, m, n_blocks)
            pltpu.make_async_copy(state.at[m], state.at[m], prev_send.at[m]).wait()
            pltpu.make_async_copy(pin.at[0, m], pin.at[0, m], po_send.at[m]).wait()

        @pl.when(s > 0)
        def _():
            pltpu.make_async_copy(state.at[m], state.at[m], out_send.at[m]).wait()

        @pl.when(in_feat)
        def _():
            pltpu.make_async_copy(rs_in.at[m], rs_in.at[m], rs_send.at[m]).wait()

        @pl.when(out_feat)
        def _():
            others = att.at[m, pl.ds(0, n_col - 1)]
            pltpu.make_async_copy(others, others, att_send.at[m]).wait()

        return carry

    lax.fori_loop(0, micro, finish, 0)


def solution(mesh):
    n_sec, n_row, n_col = mesh.shape["section"], mesh.shape["row"], mesh.shape["col"]

    def shards(hidden, norm_gain, w_qkv, w_out, cache_keys, cache_values, cache_lengths):
        micro, batch, feats = hidden.shape
        wq = w_qkv[0]
        wo = w_out[0]
        width = wq.shape[1]
        _, _, seqs, length, groups, hd = cache_keys.shape
        keys = cache_keys.reshape(micro, seqs, length, hd)
        vals = cache_values.reshape(micro, seqs, length, hd)
        rows8 = HEADS // KVH * seqs
        bf, f32 = jnp.bfloat16, jnp.float32
        vmem = pl.BlockSpec(memory_space=pltpu.VMEM)
        hbm = pl.BlockSpec(memory_space=pltpu.HBM)
        sem = pltpu.SemaphoreType.DMA
        out = pl.pallas_call(
            functools.partial(kernel, (n_sec, n_row, n_col)),
            out_shape=jax.ShapeDtypeStruct((micro, batch, feats), bf),
            in_specs=[hbm] * 7,
            out_specs=vmem,
            scratch_shapes=[
                pltpu.SMEM((seqs, micro), jnp.int32),
                pltpu.VMEM(hidden.shape, bf),
                pltpu.VMEM(norm_gain.shape, bf),
                pltpu.VMEM((n_col * feats, width), bf),
                pltpu.VMEM((n_col, *wo.shape), bf),
                pltpu.VMEM(keys.shape, bf),
                pltpu.VMEM(vals.shape, bf),
                pltpu.VMEM((micro, rows8, hd), f32),
                pltpu.VMEM((micro, rows8, hd), f32),
                pltpu.VMEM((n_col, 1, feats), bf),
                pltpu.VMEM((batch, feats), f32),
                pltpu.VMEM((micro, batch, feats), bf),
                pltpu.VMEM((micro, n_col, seqs, feats), bf),
                pltpu.VMEM((micro, n_col, seqs, feats), bf),
                pltpu.VMEM((micro, n_col, seqs, feats), bf),
                pltpu.VMEM((2, micro, n_row, batch, feats), bf),
                pltpu.VMEM((micro, n_col, seqs, width + hd), f32),
                pltpu.VMEM((micro, n_col - 1, seqs, width + hd), f32),
                pltpu.VMEM((seqs, width + hd), f32),
                pltpu.VMEM((micro, n_col, seqs, wo.shape[0]), bf),
                pltpu.VMEM((micro, batch, feats), bf),
                sem((7,)),
                sem,
                sem((2, n_col // 2, CHUNKS)),
                sem,
                sem((2, n_col // 2, CHUNKS)),
                sem,
                sem,
                pltpu.SemaphoreType.REGULAR,
                sem((micro,)),
                sem((micro,)),
                sem((micro,)),
                sem((micro,)),
                sem((micro,)),
                sem((2, micro)),
                sem((micro,)),
                sem((micro,)),
                sem((micro,)),
                sem((micro,)),
            ],
            compiler_params=pltpu.CompilerParams(
                collective_id=0, has_side_effects=True, vmem_limit_bytes=67000000
            ),
        )(cache_lengths.T, hidden, norm_gain, wq, wo, keys, vals)
        return out[None]

    return jax.shard_map(
        shards,
        mesh=mesh,
        in_specs=(
            P(None, None, "col"),
            P("section", "col"),
            P("section", "col", "row"),
            P("section", "row", "col"),
            P("section", None, "col", None, "row", None),
            P("section", None, "col", None, "row", None),
            P(None, "col"),
        ),
        out_specs=P("section", None, None, "col"),
        check_vma=False,
    )
```
